32 devices in a mesh: lat: 4 (over z), lon: 8 (over y, x, core).
Axes of the slice: x: 2, y: 2, z: 4, core: 2. Of those that a mesh axis runs over, the one named last changes fastest.
Arguments:
- fields: float32 [32, 2880, 384], P('lat', 'lon'), may hold values from -6 to 6
- cutoff: int32 [32], P('lat'), may hold values from 1 to 1395, as said below
Outputs:
- filtered: float32 [32, 2880, 384], P('lat', 'lon')
The draws below stay inside these ranges and needn't reach their ends.
Inputs may be any that keep to these rules, and one draw needn't show every extreme that they name: cutoff[g] lies between 1 and 1 + (1439)(2 p + 1) // 32, where p is the number of rows between row g and the nearer pole; this ceiling grows from the pole rows to the equator.
All inputs are finite; a program needn't handle non-finite values.
Results may differ from the reference program's by a relative error of at most 0.0003.
Values sent between devices are 32-bit elements; how exact they have to be, the bound alone decides.
A program may use at most 64 MiB of HBM per device.

```python
import jax
import jax.numpy as jnp
from jax import lax

NLON = 2880
FIELDS = 6
LEVELS = 64
NLAT = 32


def draw_cutoff(key, part):
    row_id = jnp.arange(NLAT, dtype=jnp.int32)
    pole_rows = jnp.minimum(row_id, NLAT - 1 - row_id)
    highest_cut = 1 + (NLON // 2 - 1) * (2 * pole_rows + 1) // NLAT
    drawn = jax.random.randint(key, (NLAT,), 1, highest_cut + 1, dtype=jnp.int32)
    drawn = drawn.at[NLAT // 2].set(highest_cut[NLAT // 2])
    drawn = drawn.at[NLAT - 1].set(1)
    return drawn


def block_levels(key, dims, split, smallest, top_value):
    level = 1.0
    for dim, shards_of in split:
        draws = jax.random.uniform(jax.random.fold_in(jax.random.fold_in(key, 6), dim), (shards_of,), jnp.float32, smallest / len(split), top_value / len(split))
        level = level * jnp.repeat(jnp.exp(draws), dims[dim] // shards_of).reshape((-1,) + (1,) * (len(dims) - 1 - dim))
    return level


def scatter_about(own_key, shape, scale, limit, split=(), kind=jnp.bfloat16):
    gain = block_levels(own_key, shape, split, -0.22, 0.18) if split else 1.0
    array = jax.random.normal(own_key, shape, jnp.float32) * scale * gain
    return jnp.minimum(jnp.maximum(array, -limit), limit).astype(kind)


def setup_inputs(seed: int = 0) -> dict:
    streams_of = jax.random.split(jax.random.key(seed), 3)
    fields = scatter_about(streams_of[0], (NLAT, NLON, FIELDS * LEVELS), 1.0, 6.0, ((0, 4), (1, 8)), jnp.float32)
    cutoff = draw_cutoff(jax.random.fold_in(streams_of[2], 71), 0)
    return {"fields": fields, "cutoff": cutoff}


def polar_mask(total_rows):
    latitude_row = jnp.arange(total_rows, dtype=jnp.int32)
    offset_twice = jnp.abs(2 * latitude_row + 1 - total_rows)
    return offset_twice * 5 > 2 * total_rows


def damping_row(cutoff_row, length):
    wavenumber = jnp.arange(length // 2 + 1, dtype=jnp.int32)
    cutoff_float = cutoff_row.astype(jnp.float32)
    wave_float = jnp.maximum(wavenumber, 1).astype(jnp.float32)
    ratio_value = jnp.sin(jnp.pi * cutoff_float / length) / jnp.sin(jnp.pi * wave_float / length)
    return jnp.where(wavenumber <= cutoff_row, 1.0, ratio_value * ratio_value).astype(jnp.float32)


def reference(fields, cutoff):
    total_rows = fields.shape[0]
    length = fields.shape[1]
    polar_rows = polar_mask(total_rows)

    def filter_row(packed):
        row_field, row_cutoff, row_polar = packed
        spectrum = jnp.fft.rfft(row_field, axis=0)
        scaled = spectrum * damping_row(row_cutoff, length)[:, None]
        smoothed = jnp.fft.irfft(scaled, n=length, axis=0).astype(jnp.float32)
        return jnp.where(row_polar, smoothed, row_field)

    return lax.map(filter_row, (fields, cutoff, polar_rows))
```

```python
import functools

import jax
import jax.numpy as jnp
import numpy as np
from jax import lax
from jax.experimental import pallas as pl
from jax.experimental.pallas import tpu as pltpu
from jax.sharding import PartitionSpec as P

LANES = 128
SHAPES = 15
SLOT = 2 * SHAPES + 2
PER_TILE = LANES // SLOT
NEAR_RANK, FAR_RANK = 12, 4
MESH = pl.DeviceIdType.MESH


def filter_lines(cuts, length):
    wave = np.arange(length)
    folded = np.minimum(wave, length - wave)
    sine = np.sin(np.pi * np.maximum(folded, 1) / length)
    cuts = np.asarray(cuts)[:, None]
    gain = np.where(folded[None] <= cuts, 1.0, (np.sin(np.pi * cuts / length) / sine[None]) ** 2)
    return np.fft.ifft(gain, axis=1).real


def hankel(line, segment, distance):
    first = segment * distance - (segment - 1)
    wrapped = np.take(line, np.arange(first, first + 2 * segment - 1), mode="wrap")
    return np.lib.stride_tricks.sliding_window_view(wrapped, segment)


def envelope_shapes(length, segment, top):
    spot = np.arange(segment)
    family = [(a / (spot + a)) ** p for a in np.geomspace(0.3, 2 * segment, 40) for p in (1, 2, 3)]
    unit = 2.0 * spot / (segment - 1) - 1.0
    family += [np.polynomial.chebyshev.chebval(unit, [0] * j + [1]) for j in range(8)]
    left, size, _ = np.linalg.svd(np.array(family).T, full_matrices=False)
    left = left[:, size > 1e-6 * size[0]]
    cuts = np.unique(np.round(np.geomspace(1, top, 40)).astype(int))
    parts = []
    for cut, line in zip(cuts, filter_lines(cuts, length)):
        turn = 2.0 * np.pi * cut / length * spot[:, None]
        both = np.concatenate([left * np.cos(turn), left * np.sin(turn)], axis=1)
        u, s, vt = np.linalg.svd(both, full_matrices=False)
        keep = s > 1e-5 * s[0]
        inverse = (vt[keep].T / s[keep]) @ u[:, keep].T
        for distance in range(1, min(length // segment // 2, 4) + 1):
            u, s, _ = np.linalg.svd(inverse @ hankel(line, segment, distance), full_matrices=False)
            scaled = (u * s)[:, s > 1e-7]
            parts += [scaled[: left.shape[1]], scaled[left.shape[1] :]]
    u, _, _ = np.linalg.svd(np.concatenate(parts, axis=1), full_matrices=False)
    shapes = left @ u[:, :SHAPES]
    return np.pad(shapes, ((0, 0), (0, SHAPES - shapes.shape[1])))


@functools.lru_cache(maxsize=None)
def filter_tables(length, segment, top):
    shapes = envelope_shapes(length, segment, top)
    spot = np.arange(segment)
    cuts = np.arange(1, top + 1)
    lines = filter_lines(cuts, length)
    half = length // segment // 2
    ranks = [NEAR_RANK] + [FAR_RANK] * (half - 1)
    mixing = np.zeros((-(-(top + 1) // PER_TILE), sum(ranks), LANES))
    for cut, line in zip(cuts, lines):
        turn = 2.0 * np.pi * ((cut * spot) % length)[:, None] / length
        both = np.concatenate([shapes * np.cos(turn), shapes * np.sin(turn)], axis=1)
        u, s, vt = np.linalg.svd(both, full_matrices=False)
        keep = s > 3e-4 * s[0]
        u, back = u[:, keep], vt[keep].T / s[keep]
        at, start = (cut % PER_TILE) * SLOT, 0
        for distance, rank in enumerate(ranks, 1):
            inner = u.T @ (hankel(line, segment, distance) @ u)
            size, vectors = np.linalg.eigh((inner + inner.T) / 2.0)
            order = np.argsort(-np.abs(size), kind="stable")[:rank]
            count = len(order)
            weights = (back @ vectors[:, order]).T
            here = mixing[cut // PER_TILE, start : start + count, at : at + SLOT]
            here[:, :SHAPES] = weights[:, :SHAPES]
            here[:, SHAPES + 1 : 2 * SHAPES + 1] = weights[:, SHAPES:]
            here[:, SHAPES] = size[order]
            start += rank
    padded = -(-segment // LANES) * LANES
    away = np.abs(np.arange(2 * padded) - (padded - 1))
    mirrored = np.concatenate([np.zeros((1, 2 * padded)), lines[:, away]], axis=0)
    bank = np.zeros((2, SHAPES + 1, padded))
    bank[0, :SHAPES, :segment] = shapes.T
    bank[1, :SHAPES, :segment] = shapes[::-1].T
    return mirrored.astype(np.float32), mixing.astype(np.float32), bank.astype(np.float32), ranks


def split(a):
    hi = a.astype(jnp.bfloat16)
    lo = (a - hi.astype(jnp.float32)).astype(jnp.bfloat16)
    return hi, lo


def polar_row(band, bands, rows, i):
    total = rows * bands
    return jnp.abs(2 * (band * rows + i) + 1 - total) * 5 > 2 * total


class Layout:
    def __init__(self, rows, segment, channels, ring, ranks):
        self.rows, self.segment, self.channels, self.ring = rows, segment, channels, ring
        self.padded = -(-segment // LANES) * LANES
        self.half = ring // 2
        self.ranks = ranks
        self.count = sum(ranks)
        starts = np.concatenate([[0], np.cumsum(ranks)]).astype(int)
        plus = [(d, self.count + starts[d - 1], starts[d - 1], ranks[d - 1]) for d in range(1, self.half + 1)]
        minus = [(ring - d, starts[d - 1], self.count + starts[d - 1], ranks[d - 1]) for d in range(1, self.half)]
        self.peers, at = [], 0
        for step, send_row, come_row, rank in plus + minus:
            self.peers.append((step, int(send_row), int(come_row), rank, at))
            at += rank * rows
        self.total = at


def exchange_kernel(lay, bands, x_hbm, cut_ref, line_ref, mix_ref, bank_ref, y_hbm, come_ref, m_ref, x_buf, y_buf, send, xs, x_sem, y_sem, send_sem, recv_sem):
    seg, pad, ring, pairs = lay.segment, lay.padded, lay.ring, lay.rows // 2
    band, me = lax.axis_index("lat"), lax.axis_index("lon")
    barrier = pltpu.get_barrier_semaphore()
    length = seg * ring

    def fetch(p):
        return pltpu.make_async_copy(x_hbm.at[pl.ds(2 * p, 2)], x_buf.at[pl.ds(2 * p, 2)], x_sem.at[p])

    def store(p):
        return pltpu.make_async_copy(y_buf.at[pl.ds(2 * p, 2)], y_hbm.at[pl.ds(2 * p, 2)], y_sem.at[p])

    def push(n, p):
        step, _, _, rank, at = lay.peers[n]
        rows = pl.ds(pl.multiple_of(at + 2 * rank * p, 8), 2 * rank)
        return pltpu.make_async_remote_copy(
            src_ref=send.at[rows],
            dst_ref=come_ref.at[rows],
            send_sem=send_sem.at[n, p],
            recv_sem=recv_sem.at[n, p],
            device_id={"lon": lax.rem(me + step, ring)},
            device_id_type=MESH,
        )

    for p in range(pairs):
        fetch(p).start()
    for step in range(1, ring):
        pl.semaphore_signal(barrier, inc=1, device_id={"lon": lax.rem(me + step, ring)}, device_id_type=MESH)
    xs[...] = jnp.zeros_like(xs)
    pl.semaphore_wait(barrier, ring - 1)

    spot = lax.broadcasted_iota(jnp.int32, (1, pad), 1).astype(jnp.float32)
    slot = lax.broadcasted_iota(jnp.int32, (lay.count, LANES), 1)

    def basis(cut, flip):
        turn = cut * ((seg - 1.0) - spot if flip else spot)
        turn = turn - jnp.floor(turn * (1.0 / length)) * length
        angle = turn * (2.0 * np.pi / length)
        shapes = bank_ref[int(flip)]
        both = jnp.concatenate([shapes * jnp.cos(angle), shapes * jnp.sin(angle)], axis=0)
        return jnp.concatenate([both] * PER_TILE, axis=0)

    def one(i):
        x = x_buf[i]
        hi, lo = split(x)
        xs[0:seg] = hi
        xs[pad : pad + seg] = hi
        xs[2 * pad : 2 * pad + seg] = lo
        cut = cut_ref[i]
        which = lax.rem(cut, PER_TILE)
        mix = jnp.where(slot // SLOT == which, mix_ref[i], 0.0)
        size = jnp.sum(jnp.where(lax.rem(slot, SLOT) == SHAPES, mix, 0.0), axis=1, keepdims=True)
        cut = cut.astype(jnp.float32)
        dot = functools.partial(jnp.dot, precision=lax.Precision.HIGHEST, preferred_element_type=jnp.float32)
        m = jnp.concatenate([dot(mix, basis(cut, False)), dot(mix, basis(cut, True)) * size], axis=0)
        m_ref[i] = m
        hi, lo = split(m)
        wide = xs[...]
        a = jnp.dot(jnp.concatenate([hi, lo, hi], axis=1), wide, preferred_element_type=jnp.float32)
        line = jnp.broadcast_to(line_ref[pl.ds(i, 1), :], (LANES, 2 * pad))
        sheet = pltpu.roll(line, 2 * pad - (LANES - 1), 1, stride=1, stride_axis=0)[:, : 2 * pad - LANES]
        hi, lo = split(sheet)
        on = polar_row(band, bands, lay.rows, i)
        for q in range(pad // LANES):
            cols = slice(pad - LANES * (q + 1), 2 * pad - LANES * (q + 1))
            left = jnp.concatenate([hi[:, cols], lo[:, cols], hi[:, cols]], axis=1)
            rows = min(LANES, seg - q * LANES)
            y = jnp.dot(left, wide, preferred_element_type=jnp.float32)[:rows]
            block = slice(q * LANES, q * LANES + rows)
            y_buf[i, block, :] = jnp.where(on, y, x[block])
        return a

    @pl.loop(0, pairs)
    def _(p):
        fetch(p).wait()
        first, second = one(2 * p), one(2 * p + 1)
        for n, (_, row, _, rank, at) in enumerate(lay.peers):
            both = jnp.concatenate([first[row : row + rank], second[row : row + rank]], axis=0)
            send[pl.ds(pl.multiple_of(at + 2 * rank * p, 8), 2 * rank), :] = both
        for n in range(ring - 1):
            push(n, p).start()
        store(p).start()

    @pl.loop(0, pairs)
    def _(p):
        store(p).wait()
        for n in range(ring - 1):
            push(n, p).wait()


def join_kernel(lay, bands, y_ref, come_ref, m_ref, out_ref):
    p = pl.program_id(0)
    band = lax.axis_index("lat")
    for r in range(2):
        parts = [None] * (2 * lay.count)
        for _, _, row, rank, at in lay.peers:
            both = come_ref[pl.ds(pl.multiple_of(at + 2 * rank * p, 8), 2 * rank), :]
            parts[row] = both[r * rank : (r + 1) * rank]
        gap = 2 * lay.count - sum(v.shape[0] for v in parts if v is not None)
        last = lay.count + sum(lay.ranks[:-1])
        parts[last] = jnp.zeros((gap, lay.channels), jnp.float32)
        b = jnp.concatenate([v for v in parts if v is not None], axis=0)
        m_hi, m_lo = split(m_ref[r])
        b_hi, b_lo = split(b)
        left = jnp.concatenate([m_hi, m_lo, m_hi], axis=0)
        right = jnp.concatenate([b_hi, b_hi, b_lo], axis=0)
        far = lax.dot_general(left, right, (((0,), (0,)), ((), ())), preferred_element_type=jnp.float32)
        y = y_ref[r]
        out_ref[r] = jnp.where(polar_row(band, bands, lay.rows, 2 * p + r), y + far[: lay.segment], y)


def local(ring, bands, fields, cutoff):
    rows, segment, channels = fields.shape
    length, total = ring * segment, rows * bands
    row_ids = np.arange(total)
    polar = np.abs(2 * row_ids + 1 - total) * 5 > 2 * total
    poles = np.minimum(row_ids, total - 1 - row_ids)
    top = int(1 + (length // 2 - 1) * (2 * poles[polar].max() + 1) // total)
    lines, mixing, bank, ranks = filter_tables(length, segment, top)
    lay = Layout(rows, segment, channels, ring, ranks)
    pad = lay.padded
    cut = jnp.clip(cutoff, 1, top)
    line = jnp.asarray(lines)[cut]
    mix = jnp.asarray(mixing)[cut // PER_TILE]
    f32 = jnp.float32
    any_space = pl.BlockSpec(memory_space=pl.ANY)
    vmem = pl.BlockSpec(memory_space=pltpu.VMEM)
    partial, come, m = pl.pallas_call(
        functools.partial(exchange_kernel, lay, bands),
        out_shape=[
            jax.ShapeDtypeStruct(fields.shape, f32),
            jax.ShapeDtypeStruct((lay.total, channels), f32),
            jax.ShapeDtypeStruct((rows, 2 * lay.count, pad), f32),
        ],
        in_specs=[any_space, pl.BlockSpec(memory_space=pltpu.SMEM), vmem, vmem, vmem],
        out_specs=[any_space, vmem, vmem],
        scratch_shapes=[
            pltpu.VMEM(fields.shape, f32),
            pltpu.VMEM(fields.shape, f32),
            pltpu.VMEM((lay.total, channels), f32),
            pltpu.VMEM((3 * pad, channels), jnp.bfloat16),
            pltpu.SemaphoreType.DMA((rows // 2,)),
            pltpu.SemaphoreType.DMA((rows // 2,)),
            pltpu.SemaphoreType.DMA((ring - 1, rows // 2)),
            pltpu.SemaphoreType.DMA((ring - 1, rows // 2)),
        ],
        compiler_params=pltpu.CompilerParams(collective_id=0, has_side_effects=True, vmem_limit_bytes=40 * 1024 * 1024),
        name="exchange",
    )(fields, cut, line, mix, bank)
    by_pair = lambda a: pl.BlockSpec((2,) + a.shape[1:], lambda p: (p, 0, 0))
    return pl.pallas_call(
        functools.partial(join_kernel, lay, bands),
        out_shape=jax.ShapeDtypeStruct(fields.shape, fields.dtype),
        grid=(rows // 2,),
        in_specs=[by_pair(partial), pl.BlockSpec(come.shape, lambda p: (0, 0)), by_pair(m)],
        out_specs=by_pair(fields),
        compiler_params=pltpu.CompilerParams(vmem_limit_bytes=40 * 1024 * 1024),
        name="join",
    )(partial, come, m)


def solution(mesh):
    return jax.shard_map(
        functools.partial(local, mesh.shape["lon"], mesh.shape["lat"]),
        mesh=mesh,
        in_specs=(P("lat", "lon", None), P("lat")),
        out_specs=P("lat", "lon", None),
        check_vma=False,
    )
```

```python
import functools

import jax
import jax.numpy as jnp
import numpy as np
from jax import lax
from jax.experimental import pallas as pl
from jax.experimental.pallas import tpu as pltpu
from jax.sharding import PartitionSpec as P

LANES = 128
SHAPES = 15
SLOT = 2 * SHAPES + 2
PER_TILE = LANES // SLOT
NEAR_RANK, FAR_RANK = 12, 4
MESH = pl.DeviceIdType.MESH


def filter_lines(cuts, length):
    wave = np.arange(length)
    folded = np.minimum(wave, length - wave)
    sine = np.sin(np.pi * np.maximum(folded, 1) / length)
    cuts = np.asarray(cuts)[:, None]
    gain = np.where(folded[None] <= cuts, 1.0, (np.sin(np.pi * cuts / length) / sine[None]) ** 2)
    return np.fft.ifft(gain, axis=1).real


def hankel(line, segment, distance):
    first = segment * distance - (segment - 1)
    wrapped = np.take(line, np.arange(first, first + 2 * segment - 1), mode="wrap")
    return np.lib.stride_tricks.sliding_window_view(wrapped, segment)


def envelope_shapes(length, segment, top):
    spot = np.arange(segment)
    family = [(a / (spot + a)) ** p for a in np.geomspace(0.3, 2 * segment, 40) for p in (1, 2, 3)]
    unit = 2.0 * spot / (segment - 1) - 1.0
    family += [np.polynomial.chebyshev.chebval(unit, [0] * j + [1]) for j in range(8)]
    left, size, _ = np.linalg.svd(np.array(family).T, full_matrices=False)
    left = left[:, size > 1e-6 * size[0]]
    cuts = np.unique(np.round(np.geomspace(1, top, 40)).astype(int))
    parts = []
    for cut, line in zip(cuts, filter_lines(cuts, length)):
        turn = 2.0 * np.pi * cut / length * spot[:, None]
        both = np.concatenate([left * np.cos(turn), left * np.sin(turn)], axis=1)
        u, s, vt = np.linalg.svd(both, full_matrices=False)
        keep = s > 1e-5 * s[0]
        inverse = (vt[keep].T / s[keep]) @ u[:, keep].T
        for distance in range(1, min(length // segment // 2, 4) + 1):
            u, s, _ = np.linalg.svd(inverse @ hankel(line, segment, distance), full_matrices=False)
            scaled = (u * s)[:, s > 1e-7]
            parts += [scaled[: left.shape[1]], scaled[left.shape[1] :]]
    u, _, _ = np.linalg.svd(np.concatenate(parts, axis=1), full_matrices=False)
    shapes = left @ u[:, :SHAPES]
    return np.pad(shapes, ((0, 0), (0, SHAPES - shapes.shape[1])))


@functools.lru_cache(maxsize=None)
def filter_tables(length, segment, top):
    shapes = envelope_shapes(length, segment, top)
    spot = np.arange(segment)
    cuts = np.arange(1, top + 1)
    lines = filter_lines(cuts, length)
    half = length // segment // 2
    ranks = [NEAR_RANK] + [FAR_RANK] * (half - 1)
    mixing = np.zeros((-(-(top + 1) // PER_TILE), sum(ranks), LANES))
    for cut, line in zip(cuts, lines):
        turn = 2.0 * np.pi * ((cut * spot) % length)[:, None] / length
        both = np.concatenate([shapes * np.cos(turn), shapes * np.sin(turn)], axis=1)
        u, s, vt = np.linalg.svd(both, full_matrices=False)
        keep = s > 3e-4 * s[0]
        u, back = u[:, keep], vt[keep].T / s[keep]
        at, start = (cut % PER_TILE) * SLOT, 0
        for distance, rank in enumerate(ranks, 1):
            inner = u.T @ (hankel(line, segment, distance) @ u)
            size, vectors = np.linalg.eigh((inner + inner.T) / 2.0)
            order = np.argsort(-np.abs(size), kind="stable")[:rank]
            count = len(order)
            weights = (back @ vectors[:, order]).T
            here = mixing[cut // PER_TILE, start : start + count, at : at + SLOT]
            here[:, :SHAPES] = weights[:, :SHAPES]
            here[:, SHAPES + 1 : 2 * SHAPES + 1] = weights[:, SHAPES:]
            here[:, SHAPES] = size[order]
            start += rank
    padded = -(-segment // LANES) * LANES
    away = np.abs(np.arange(2 * padded) - (padded - 1))
    tiles = -(-2 * padded // LANES // 8) * 8
    mirrored = np.zeros((mixing.shape[0] * PER_TILE, tiles * LANES))
    mirrored[1 : top + 1, : 2 * padded] = lines[:, away]
    table = np.concatenate([mirrored.reshape(-1, PER_TILE * tiles, LANES), mixing], axis=1)
    tail = np.zeros((2,) + table.shape[1:])
    for flip in range(2):
        bank = np.zeros((SHAPES + 1, padded))
        bank[:SHAPES, :segment] = (shapes[::-1] if flip else shapes).T
        for k in range(padded // LANES):
            tail[flip, k * (SHAPES + 1) : (k + 1) * (SHAPES + 1)] = bank[:, k * LANES : (k + 1) * LANES]
    table = np.concatenate([table, tail], axis=0)
    return table.astype(np.float32), tiles, ranks


def split(a):
    hi = a.astype(jnp.bfloat16)
    lo = (a - hi.astype(jnp.float32)).astype(jnp.bfloat16)
    return hi, lo


def polar_row(band, bands, rows, i):
    total = rows * bands
    return jnp.abs(2 * (band * rows + i) + 1 - total) * 5 > 2 * total


class Layout:
    def __init__(self, rows, segment, channels, ring, ranks):
        self.rows, self.segment, self.channels, self.ring = rows, segment, channels, ring
        self.padded = -(-segment // LANES) * LANES
        self.half = ring // 2
        self.tall = -(-(2 * sum(ranks) + segment) // 16) * 16
        self.ranks = ranks
        self.count = sum(ranks)
        starts = np.concatenate([[0], np.cumsum(ranks)]).astype(int)
        plus = [(d, self.count + starts[d - 1], starts[d - 1], ranks[d - 1]) for d in range(1, self.half + 1)]
        minus = [(ring - d, starts[d - 1], self.count + starts[d - 1], ranks[d - 1]) for d in range(1, self.half)]
        self.peers, at = [], 0
        for step, send_row, come_row, rank in plus + minus:
            self.peers.append((step, int(send_row), int(come_row), rank, at))
            at += rank * rows
        self.total = at


def three(a):
    hi = a.astype(jnp.bfloat16)
    rest = a - hi.astype(jnp.float32)
    mid = rest.astype(jnp.bfloat16)
    return hi, mid, (rest - mid.astype(jnp.float32)).astype(jnp.bfloat16)


def lookup_kernel(lay, top, cut_ref, table_hbm, line_ref, left_ref, bank_buf, mix_buf, bank_sem, line_sem, mix_sem):
    rows, seg, pad, length = lay.rows, lay.segment, lay.padded, lay.segment * lay.ring
    tiles = line_ref.shape[1]
    cuts = [jnp.clip(cut_ref[i], 1, top) for i in range(rows)]
    lines, mixes = [], []
    shapes = pltpu.make_async_copy(table_hbm.at[pl.ds(table_hbm.shape[0] - 2, 2), pl.ds(0, bank_buf.shape[1])], bank_buf, bank_sem)
    shapes.start()
    for i in range(rows):
        group = table_hbm.at[cuts[i] // PER_TILE]
        start = pl.multiple_of(lax.rem(cuts[i], PER_TILE) * tiles, 8)
        mixes.append(pltpu.make_async_copy(group.at[pl.ds(PER_TILE * tiles, lay.count)], mix_buf.at[i], mix_sem.at[i]))
        lines.append(pltpu.make_async_copy(group.at[pl.ds(start, tiles)], line_ref.at[i], line_sem.at[i]))
    for copy in mixes + lines:
        copy.start()

    row = lax.broadcasted_iota(jnp.int32, (rows, pad), 0)
    spot = lax.broadcasted_iota(jnp.int32, (rows, pad), 1).astype(jnp.float32)
    cut = functools.reduce(lambda v, i: jnp.where(row == i, cuts[i].astype(jnp.float32), v), range(rows), jnp.zeros((rows, pad), jnp.float32))

    def waves(turn):
        turn = turn - jnp.floor(turn * (1.0 / length)) * length
        angle = turn * (2.0 * np.pi / length)
        return jnp.cos(angle), jnp.sin(angle)

    ahead, behind = waves(cut * spot), waves(cut * ((seg - 1.0) - spot))
    slot = lax.broadcasted_iota(jnp.int32, (lay.count, LANES), 1)
    shapes.wait()
    step = SHAPES + 1
    bank = [jnp.concatenate([bank_buf[f, k * step : (k + 1) * step] for k in range(pad // LANES)], axis=1) for f in range(2)]
    for i in range(rows):
        basis = [jnp.concatenate([bank[f] * w[i : i + 1] for w in pair], axis=0) for f, pair in enumerate((ahead, behind))]
        hi, mid, lo = three(jnp.concatenate(basis, axis=1))
        right = jnp.concatenate([hi, mid, lo, hi, mid, hi], axis=0)
        mixes[i].wait()
        mix = jnp.where(slot // SLOT == lax.rem(cuts[i], PER_TILE), mix_buf[i], 0.0)
        size = jnp.sum(jnp.where(lax.rem(slot, SLOT) == SHAPES, mix, 0.0), axis=1, keepdims=True)
        mix = functools.reduce(jnp.add, [mix[:, k * SLOT : (k + 1) * SLOT] for k in range(PER_TILE)])
        hi, mid, lo = three(mix)
        left = jnp.concatenate([hi, hi, hi, mid, mid, lo], axis=1)
        q = jnp.dot(left, right, preferred_element_type=jnp.float32)
        hi, lo = split(jnp.concatenate([q[:, :pad], q[:, pad:] * size], axis=0))
        left_ref[i] = jnp.concatenate([hi, lo, hi], axis=1)
    for copy in lines:
        copy.wait()


def exchange_kernel(lay, bands, x_ref, line_ref, left_ref, y_ref, come_ref, send, xs, left, send_sem, recv_sem):
    seg, pad, ring, pairs = lay.segment, lay.padded, lay.ring, lay.rows // 2
    tops = 2 * lay.count
    band, me = lax.axis_index("lat"), lax.axis_index("lon")
    barrier = pltpu.get_barrier_semaphore()

    def push(n, p):
        step, _, _, rank, at = lay.peers[n]
        rows = pl.ds(pl.multiple_of(at + 2 * rank * p, 8), 2 * rank)
        return pltpu.make_async_remote_copy(
            src_ref=send.at[rows],
            dst_ref=come_ref.at[rows],
            send_sem=send_sem.at[n, p],
            recv_sem=recv_sem.at[n, p],
            device_id={"lon": lax.rem(me + step, ring)},
            device_id_type=MESH,
        )

    for step in range(1, ring):
        pl.semaphore_signal(barrier, inc=1, device_id={"lon": lax.rem(me + step, ring)}, device_id_type=MESH)
    xs[...] = jnp.zeros_like(xs)

    def one(i, s):
        x = x_ref[i]
        hi, lo = split(x)
        xs[s, 0:seg] = hi
        xs[s, pad : pad + seg] = hi
        xs[s, 2 * pad : 2 * pad + seg] = lo
        left[s, 0:tops] = left_ref[i]
        line = line_ref[i]
        line = jnp.concatenate([jnp.broadcast_to(line[k : k + 1], (LANES, LANES)) for k in range(2 * pad // LANES)], axis=1)
        sheet = pltpu.roll(line, 2 * pad - (LANES - 1), 1, stride=1, stride_axis=0)[:, : 2 * pad - LANES]
        hi, lo = split(sheet)
        for q in range(pad // LANES):
            cols = slice(pad - LANES * (q + 1), 2 * pad - LANES * (q + 1))
            rows = min(LANES, lay.tall - tops - q * LANES)
            block = slice(tops + q * LANES, tops + q * LANES + rows)
            left[s, block, 0:pad] = hi[:rows, cols]
            left[s, block, pad : 2 * pad] = lo[:rows, cols]
            left[s, block, 2 * pad : 3 * pad] = hi[:rows, cols]
        both = jnp.dot(left[s], xs[s], preferred_element_type=jnp.float32)
        y_ref[i] = jnp.where(polar_row(band, bands, lay.rows, i), both[tops : tops + seg], x)
        return both[:tops]

    @pl.loop(0, pairs)
    def _(p):
        first, second = one(2 * p, 0), one(2 * p + 1, 1)
        for _, row, _, rank, at in lay.peers:
            both = jnp.concatenate([first[row : row + rank], second[row : row + rank]], axis=0)
            send[pl.ds(pl.multiple_of(at + 2 * rank * p, 8), 2 * rank), :] = both

        @pl.when(p == 0)
        def _():
            pl.semaphore_wait(barrier, ring - 1)

        for n in range(ring - 1):
            push(n, p).start()

    @pl.loop(0, pairs)
    def _(p):
        for n in range(ring - 1):
            push(n, p).wait()


def join_kernel(lay, bands, y_ref, come_ref, m_ref, out_ref):
    p = pl.program_id(0)
    band = lax.axis_index("lat")
    for r in range(2):
        parts = [None] * (2 * lay.count)
        for _, _, row, rank, at in lay.peers:
            both = come_ref[pl.ds(pl.multiple_of(at + 2 * rank * p, 8), 2 * rank), :]
            parts[row] = both[r * rank : (r + 1) * rank]
        gap = 2 * lay.count - sum(v.shape[0] for v in parts if v is not None)
        last = lay.count + sum(lay.ranks[:-1])
        parts[last] = jnp.zeros((gap, lay.channels), jnp.float32)
        b = jnp.concatenate([v for v in parts if v is not None], axis=0)
        pad = lay.padded
        b_hi, b_lo = split(b)
        left = jnp.concatenate([m_ref[r, :, k * pad : (k + 1) * pad] for k in range(3)], axis=0)
        right = jnp.concatenate([b_hi, b_hi, b_lo], axis=0)
        far = lax.dot_general(left, right, (((0,), (0,)), ((), ())), preferred_element_type=jnp.float32)
        y = y_ref[r]
        out_ref[r] = jnp.where(polar_row(band, bands, lay.rows, 2 * p + r), y + far[: lay.segment], y)


def local(ring, bands, fields, cutoff):
    rows, segment, channels = fields.shape
    length, total = ring * segment, rows * bands
    row_ids = np.arange(total)
    polar = np.abs(2 * row_ids + 1 - total) * 5 > 2 * total
    poles = np.minimum(row_ids, total - 1 - row_ids)
    top = int(1 + (length // 2 - 1) * (2 * poles[polar].max() + 1) // total)
    table, tiles, ranks = filter_tables(length, segment, top)
    lay = Layout(rows, segment, channels, ring, ranks)
    pad = lay.padded
    f32 = jnp.float32
    hbm = pl.BlockSpec(memory_space=pltpu.HBM)
    vmem = pl.BlockSpec(memory_space=pltpu.VMEM)
    params = functools.partial(pltpu.CompilerParams, vmem_limit_bytes=24 * 1024 * 1024)
    line, left = pl.pallas_call(
        functools.partial(lookup_kernel, lay, top),
        out_shape=[
            jax.ShapeDtypeStruct((rows, tiles, LANES), f32),
            jax.ShapeDtypeStruct((rows, 2 * lay.count, 3 * pad), jnp.bfloat16),
        ],
        in_specs=[pl.BlockSpec(memory_space=pltpu.SMEM), hbm],
        out_specs=[vmem, vmem],
        scratch_shapes=[
            pltpu.VMEM((2, (SHAPES + 1) * pad // LANES, LANES), f32),
            pltpu.VMEM((rows, lay.count, LANES), f32),
            pltpu.SemaphoreType.DMA,
            pltpu.SemaphoreType.DMA((rows,)),
            pltpu.SemaphoreType.DMA((rows,)),
        ],
        compiler_params=pltpu.CompilerParams(vmem_limit_bytes=52 * 1024 * 1024),
        name="lookup",
    )(cutoff, table)
    partial, come = pl.pallas_call(
        functools.partial(exchange_kernel, lay, bands),
        out_shape=[
            jax.ShapeDtypeStruct(fields.shape, f32),
            jax.ShapeDtypeStruct((lay.total, channels), f32),
        ],
        in_specs=[vmem, vmem, vmem],
        out_specs=[vmem, vmem],
        scratch_shapes=[
            pltpu.VMEM((lay.total, channels), f32),
            pltpu.VMEM((2, 3 * pad, channels), jnp.bfloat16),
            pltpu.VMEM((2, lay.tall, 3 * pad), jnp.bfloat16),
            pltpu.SemaphoreType.DMA((ring - 1, rows // 2)),
            pltpu.SemaphoreType.DMA((ring - 1, rows // 2)),
        ],
        compiler_params=params(collective_id=0, has_side_effects=True),
        name="exchange",
    )(fields, line, left)
    by_pair = lambda a: pl.BlockSpec((2,) + a.shape[1:], lambda p: (p, 0, 0))
    return pl.pallas_call(
        functools.partial(join_kernel, lay, bands),
        out_shape=jax.ShapeDtypeStruct(fields.shape, fields.dtype),
        grid=(rows // 2,),
        in_specs=[by_pair(partial), pl.BlockSpec(come.shape, lambda p: (0, 0)), by_pair(left)],
        out_specs=by_pair(fields),
        compiler_params=params(),
        name="join",
    )(partial, come, left)


def solution(mesh):
    return jax.shard_map(
        functools.partial(local, mesh.shape["lon"], mesh.shape["lat"]),
        mesh=mesh,
        in_specs=(P("lat", "lon", None), P("lat")),
        out_specs=P("lat", "lon", None),
        check_vma=False,
    )
```

```python
import functools

import jax
import jax.numpy as jnp
import numpy as np
from jax import lax
from jax.experimental import pallas as pl
from jax.experimental.pallas import tpu as pltpu
from jax.sharding import PartitionSpec as P

LANES = 128
SHAPES = 15
SLOT = 2 * SHAPES + 2
PER_TILE = LANES // SLOT
NEAR_RANK, FAR_RANK = 12, 4
MESH = pl.DeviceIdType.MESH


def filter_lines(cuts, length):
    wave = np.arange(length)
    folded = np.minimum(wave, length - wave)
    sine = np.sin(np.pi * np.maximum(folded, 1) / length)
    cuts = np.asarray(cuts)[:, None]
    gain = np.where(folded[None] <= cuts, 1.0, (np.sin(np.pi * cuts / length) / sine[None]) ** 2)
    return np.fft.ifft(gain, axis=1).real


def hankel(line, segment, distance):
    first = segment * distance - (segment - 1)
    wrapped = np.take(line, np.arange(first, first + 2 * segment - 1), mode="wrap")
    return np.lib.stride_tricks.sliding_window_view(wrapped, segment)


def envelope_shapes(length, segment, top):
    spot = np.arange(segment)
    family = [(a / (spot + a)) ** p for a in np.geomspace(0.3, 2 * segment, 40) for p in (1, 2, 3)]
    unit = 2.0 * spot / (segment - 1) - 1.0
    family += [np.polynomial.chebyshev.chebval(unit, [0] * j + [1]) for j in range(8)]
    left, size, _ = np.linalg.svd(np.array(family).T, full_matrices=False)
    left = left[:, size > 1e-6 * size[0]]
    cuts = np.unique(np.round(np.geomspace(1, top, 40)).astype(int))
    parts = []
    for cut, line in zip(cuts, filter_lines(cuts, length)):
        turn = 2.0 * np.pi * cut / length * spot[:, None]
        both = np.concatenate([left * np.cos(turn), left * np.sin(turn)], axis=1)
        u, s, vt = np.linalg.svd(both, full_matrices=False)
        keep = s > 1e-5 * s[0]
        inverse = (vt[keep].T / s[keep]) @ u[:, keep].T
        for distance in range(1, min(length // segment // 2, 4) + 1):
            u, s, _ = np.linalg.svd(inverse @ hankel(line, segment, distance), full_matrices=False)
            scaled = (u * s)[:, s > 1e-7]
            parts += [scaled[: left.shape[1]], scaled[left.shape[1] :]]
    u, _, _ = np.linalg.svd(np.concatenate(parts, axis=1), full_matrices=False)
    shapes = left @ u[:, :SHAPES]
    return np.pad(shapes, ((0, 0), (0, SHAPES - shapes.shape[1])))


@functools.lru_cache(maxsize=None)
def filter_tables(length, segment, top):
    shapes = envelope_shapes(length, segment, top)
    spot = np.arange(segment)
    cuts = np.arange(1, top + 1)
    lines = filter_lines(cuts, length)
    half = length // segment // 2
    ranks = [NEAR_RANK] + [FAR_RANK] * (half - 1)
    mixing = np.zeros((-(-(top + 1) // PER_TILE), sum(ranks), LANES))
    for cut, line in zip(cuts, lines):
        turn = 2.0 * np.pi * ((cut * spot) % length)[:, None] / length
        both = np.concatenate([shapes * np.cos(turn), shapes * np.sin(turn)], axis=1)
        u, s, vt = np.linalg.svd(both, full_matrices=False)
        keep = s > 3e-4 * s[0]
        u, back = u[:, keep], vt[keep].T / s[keep]
        at, start = (cut % PER_TILE) * SLOT, 0
        for distance, rank in enumerate(ranks, 1):
            inner = u.T @ (hankel(line, segment, distance) @ u)
            size, vectors = np.linalg.eigh((inner + inner.T) / 2.0)
            order = np.argsort(-np.abs(size), kind="stable")[:rank]
            count = len(order)
            weights = (back @ vectors[:, order]).T
            here = mixing[cut // PER_TILE, start : start + count, at : at + SLOT]
            here[:, :SHAPES] = weights[:, :SHAPES]
            here[:, SHAPES + 1 : 2 * SHAPES + 1] = weights[:, SHAPES:]
            here[:, SHAPES] = size[order]
            start += rank
    padded = -(-segment // LANES) * LANES
    away = np.abs(np.arange(2 * padded) - (padded - 1))
    tiles = -(-2 * padded // LANES // 8) * 8
    mirrored = np.zeros((mixing.shape[0] * PER_TILE, tiles * LANES))
    mirrored[1 : top + 1, : 2 * padded] = lines[:, away]
    table = np.concatenate([mirrored.reshape(-1, PER_TILE * tiles, LANES), mixing], axis=1)
    tail = np.zeros((2,) + table.shape[1:])
    for flip in range(2):
        bank = np.zeros((SHAPES + 1, padded))
        bank[:SHAPES, :segment] = (shapes[::-1] if flip else shapes).T
        for k in range(padded // LANES):
            tail[flip, k * (SHAPES + 1) : (k + 1) * (SHAPES + 1)] = bank[:, k * LANES : (k + 1) * LANES]
    table = np.concatenate([table, tail], axis=0)
    return table.astype(np.float32), tiles, ranks


def split(a):
    hi = a.astype(jnp.bfloat16)
    lo = (a - hi.astype(jnp.float32)).astype(jnp.bfloat16)
    return hi, lo


def polar_row(band, bands, rows, i):
    total = rows * bands
    return jnp.abs(2 * (band * rows + i) + 1 - total) * 5 > 2 * total


class Layout:
    def __init__(self, rows, segment, channels, ring, ranks):
        self.rows, self.segment, self.channels, self.ring = rows, segment, channels, ring
        self.padded = -(-segment // LANES) * LANES
        self.half = ring // 2
        self.tall = -(-segment // 16) * 16
        self.ranks = ranks
        self.count = sum(ranks)
        starts = np.concatenate([[0], np.cumsum(ranks)]).astype(int)
        plus = [(d, self.count + starts[d - 1], starts[d - 1], ranks[d - 1]) for d in range(1, self.half + 1)]
        minus = [(ring - d, starts[d - 1], self.count + starts[d - 1], ranks[d - 1]) for d in range(1, self.half)]
        self.peers, at = [], 0
        for step, send_row, come_row, rank in plus + minus:
            self.peers.append((step, int(send_row), int(come_row), rank, at))
            at += rank * rows
        self.total = at


def three(a):
    hi = a.astype(jnp.bfloat16)
    rest = a - hi.astype(jnp.float32)
    mid = rest.astype(jnp.bfloat16)
    return hi, mid, (rest - mid.astype(jnp.float32)).astype(jnp.bfloat16)


def lookup_kernel(lay, top, cut_ref, table_hbm, line_ref, mix_ref, bank_ref, bank_sem, line_sem, mix_sem):
    rows, tiles = lay.rows, line_ref.shape[1]
    copies = [pltpu.make_async_copy(table_hbm.at[pl.ds(table_hbm.shape[0] - 2, 2), pl.ds(0, bank_ref.shape[1])], bank_ref, bank_sem)]
    for i in range(rows):
        cut = jnp.clip(cut_ref[i], 1, top)
        group = table_hbm.at[cut // PER_TILE]
        start = pl.multiple_of(lax.rem(cut, PER_TILE) * tiles, 8)
        copies.append(pltpu.make_async_copy(group.at[pl.ds(PER_TILE * tiles, lay.count)], mix_ref.at[i], mix_sem.at[i]))
        copies.append(pltpu.make_async_copy(group.at[pl.ds(start, tiles)], line_ref.at[i], line_sem.at[i]))
    for copy in copies:
        copy.start()
    for copy in copies:
        copy.wait()


def exchange_kernel(lay, bands, top, cut_ref, x_ref, line_ref, mix_ref, bank_ref, y_ref, come_ref, m_ref, send, xs, left, turns, send_sem, recv_sem):
    seg, pad, ring, pairs = lay.segment, lay.padded, lay.ring, lay.rows // 2
    length = seg * ring
    band, me = lax.axis_index("lat"), lax.axis_index("lon")
    barrier = pltpu.get_barrier_semaphore()

    def push(n, p):
        step, _, _, rank, at = lay.peers[n]
        rows = pl.ds(pl.multiple_of(at + 2 * rank * p, 8), 2 * rank)
        return pltpu.make_async_remote_copy(
            src_ref=send.at[rows],
            dst_ref=come_ref.at[rows],
            send_sem=send_sem.at[n, p],
            recv_sem=recv_sem.at[n, p],
            device_id={"lon": lax.rem(me + step, ring)},
            device_id_type=MESH,
        )

    for step in range(1, ring):
        pl.semaphore_signal(barrier, inc=1, device_id={"lon": lax.rem(me + step, ring)}, device_id_type=MESH)

    if pad != seg:
        for r in range(lay.rows):
            for k in range(3):
                xs[r, k * pad + seg : (k + 1) * pad] = jnp.zeros((pad - seg, lay.channels), jnp.bfloat16)
    row = lax.broadcasted_iota(jnp.int32, (lay.rows, pad), 0)
    spot = lax.broadcasted_iota(jnp.int32, (lay.rows, pad), 1).astype(jnp.float32)
    cut = jnp.zeros((lay.rows, pad), jnp.float32)
    for i in range(lay.rows):
        cut = jnp.where(row == i, jnp.clip(cut_ref[i], 1, top).astype(jnp.float32), cut)
    for f, place in enumerate((spot, (seg - 1.0) - spot)):
        turn = cut * place
        turn = turn - jnp.floor(turn * (1.0 / length)) * length
        angle = turn * (2.0 * np.pi / length)
        turns[2 * f] = jnp.cos(angle)
        turns[2 * f + 1] = jnp.sin(angle)
    slot = lax.broadcasted_iota(jnp.int32, (lay.count, LANES), 1)
    step = SHAPES + 1

    def project(i):
        x = x_ref[i]
        hi, lo = split(x)
        xs[i, 0:seg] = hi
        xs[i, pad : pad + seg] = hi
        xs[i, 2 * pad : 2 * pad + seg] = lo
        basis = []
        for f in range(2):
            bank = jnp.concatenate([bank_ref[f, k * step : (k + 1) * step] for k in range(pad // LANES)], axis=1)
            basis.append(jnp.concatenate([bank * turns[2 * f + w, pl.ds(i, 1), :] for w in range(2)], axis=0))
        hi, mid, lo = three(jnp.concatenate(basis, axis=1))
        right = jnp.concatenate([hi, mid, lo, hi, mid, hi], axis=0)
        mix = jnp.where(slot // SLOT == lax.rem(jnp.clip(cut_ref[i], 1, top), PER_TILE), mix_ref[i], 0.0)
        size = jnp.sum(jnp.where(lax.rem(slot, SLOT) == SHAPES, mix, 0.0), axis=1, keepdims=True)
        mix = functools.reduce(jnp.add, [mix[:, k * SLOT : (k + 1) * SLOT] for k in range(PER_TILE)])
        hi, mid, lo = three(mix)
        q = jnp.dot(jnp.concatenate([hi, hi, hi, mid, mid, lo], axis=1), right, preferred_element_type=jnp.float32)
        hi, lo = split(jnp.concatenate([q[:, :pad], q[:, pad:] * size], axis=0))
        m = jnp.concatenate([hi, lo, hi], axis=1)
        m_ref[i] = m
        return jnp.dot(m, xs[i], preferred_element_type=jnp.float32)

    def diagonal(i, s):
        line = line_ref[i]
        line = jnp.concatenate([jnp.broadcast_to(line[k : k + 1], (LANES, LANES)) for k in range(2 * pad // LANES)], axis=1)
        sheet = pltpu.roll(line, 2 * pad - (LANES - 1), 1, stride=1, stride_axis=0)[:, : 2 * pad - LANES]
        hi, lo = split(sheet)
        for q in range(pad // LANES):
            cols = slice(pad - LANES * (q + 1), 2 * pad - LANES * (q + 1))
            rows = min(LANES, lay.tall - q * LANES)
            block = slice(q * LANES, q * LANES + rows)
            left[s, block, 0:pad] = hi[:rows, cols]
            left[s, block, pad : 2 * pad] = lo[:rows, cols]
            left[s, block, 2 * pad : 3 * pad] = hi[:rows, cols]
        y = jnp.dot(left[s], xs[i], preferred_element_type=jnp.float32)[:seg]
        y_ref[i] = jnp.where(polar_row(band, bands, lay.rows, i), y, x_ref[i])

    @pl.loop(0, pairs)
    def _(p):
        first, second = project(2 * p), project(2 * p + 1)
        for _, at_row, _, rank, at in lay.peers:
            both = jnp.concatenate([first[at_row : at_row + rank], second[at_row : at_row + rank]], axis=0)
            send[pl.ds(pl.multiple_of(at + 2 * rank * p, 8), 2 * rank), :] = both

        @pl.when(p == 0)
        def _():
            pl.semaphore_wait(barrier, ring - 1)

        for n in range(ring - 1):
            push(n, p).start()

    @pl.loop(0, pairs)
    def _(p):
        diagonal(2 * p, 0)
        diagonal(2 * p + 1, 1)

    @pl.loop(0, pairs)
    def _(p):
        for n in range(ring - 1):
            push(n, p).wait()


def join_kernel(lay, bands, y_ref, come_ref, m_ref, out_ref):
    p = pl.program_id(0)
    band = lax.axis_index("lat")
    for r in range(2):
        parts = [None] * (2 * lay.count)
        for _, _, row, rank, at in lay.peers:
            both = come_ref[pl.ds(pl.multiple_of(at + 2 * rank * p, 8), 2 * rank), :]
            parts[row] = both[r * rank : (r + 1) * rank]
        gap = 2 * lay.count - sum(v.shape[0] for v in parts if v is not None)
        last = lay.count + sum(lay.ranks[:-1])
        parts[last] = jnp.zeros((gap, lay.channels), jnp.float32)
        b = jnp.concatenate([v for v in parts if v is not None], axis=0)
        pad = lay.padded
        b_hi, b_lo = split(b)
        left = jnp.concatenate([m_ref[r, :, k * pad : (k + 1) * pad] for k in range(3)], axis=0)
        right = jnp.concatenate([b_hi, b_hi, b_lo], axis=0)
        far = lax.dot_general(left, right, (((0,), (0,)), ((), ())), preferred_element_type=jnp.float32)
        y = y_ref[r]
        out_ref[r] = jnp.where(polar_row(band, bands, lay.rows, 2 * p + r), y + far[: lay.segment], y)


def local(ring, bands, fields, cutoff):
    rows, segment, channels = fields.shape
    length, total = ring * segment, rows * bands
    row_ids = np.arange(total)
    polar = np.abs(2 * row_ids + 1 - total) * 5 > 2 * total
    poles = np.minimum(row_ids, total - 1 - row_ids)
    top = int(1 + (length // 2 - 1) * (2 * poles[polar].max() + 1) // total)
    table, tiles, ranks = filter_tables(length, segment, top)
    lay = Layout(rows, segment, channels, ring, ranks)
    pad = lay.padded
    f32 = jnp.float32
    hbm = pl.BlockSpec(memory_space=pltpu.HBM)
    vmem = pl.BlockSpec(memory_space=pltpu.VMEM)
    params = functools.partial(pltpu.CompilerParams, vmem_limit_bytes=24 * 1024 * 1024)
    line, mix, bank = pl.pallas_call(
        functools.partial(lookup_kernel, lay, top),
        out_shape=[
            jax.ShapeDtypeStruct((rows, tiles, LANES), f32),
            jax.ShapeDtypeStruct((rows, lay.count, LANES), f32),
            jax.ShapeDtypeStruct((2, (SHAPES + 1) * pad // LANES, LANES), f32),
        ],
        in_specs=[pl.BlockSpec(memory_space=pltpu.SMEM), hbm],
        out_specs=[vmem] * 3,
        scratch_shapes=[
            pltpu.SemaphoreType.DMA,
            pltpu.SemaphoreType.DMA((rows,)),
            pltpu.SemaphoreType.DMA((rows,)),
        ],
        compiler_params=pltpu.CompilerParams(vmem_limit_bytes=52 * 1024 * 1024),
        name="lookup",
    )(cutoff, table)
    partial, come, left = pl.pallas_call(
        functools.partial(exchange_kernel, lay, bands, top),
        out_shape=[
            jax.ShapeDtypeStruct(fields.shape, f32),
            jax.ShapeDtypeStruct((lay.total, channels), f32),
            jax.ShapeDtypeStruct((rows, 2 * lay.count, 3 * pad), jnp.bfloat16),
        ],
        in_specs=[pl.BlockSpec(memory_space=pltpu.SMEM), vmem, vmem, vmem, vmem],
        out_specs=[vmem] * 3,
        scratch_shapes=[
            pltpu.VMEM((lay.total, channels), f32),
            pltpu.VMEM((rows, 3 * pad, channels), jnp.bfloat16),
            pltpu.VMEM((2, lay.tall, 3 * pad), jnp.bfloat16),
            pltpu.VMEM((4, rows, pad), f32),
            pltpu.SemaphoreType.DMA((ring - 1, rows // 2)),
            pltpu.SemaphoreType.DMA((ring - 1, rows // 2)),
        ],
        compiler_params=params(collective_id=0, has_side_effects=True),
        name="exchange",
    )(cutoff, fields, line, mix, bank)
    by_pair = lambda a: pl.BlockSpec((2,) + a.shape[1:], lambda p: (p, 0, 0))
    return pl.pallas_call(
        functools.partial(join_kernel, lay, bands),
        out_shape=jax.ShapeDtypeStruct(fields.shape, fields.dtype),
        grid=(rows // 2,),
        in_specs=[by_pair(partial), pl.BlockSpec(come.shape, lambda p: (0, 0)), by_pair(left)],
        out_specs=by_pair(fields),
        compiler_params=params(),
        name="join",
    )(partial, come, left)


def solution(mesh):
    return jax.shard_map(
        functools.partial(local, mesh.shape["lon"], mesh.shape["lat"]),
        mesh=mesh,
        in_specs=(P("lat", "lon", None), P("lat")),
        out_specs=P("lat", "lon", None),
        check_vma=False,
    )
```

```python
import functools

import jax
import jax.numpy as jnp
import numpy as np
from jax import lax
from jax.experimental import pallas as pl
from jax.experimental.pallas import tpu as pltpu
from jax.sharding import PartitionSpec as P

LANES = 128
SHAPES = 15
SLOT = 2 * SHAPES + 2
PER_TILE = LANES // SLOT
NEAR_RANK, FAR_RANK = 12, 4
MESH = pl.DeviceIdType.MESH


def filter_lines(cuts, length):
    wave = np.arange(length)
    folded = np.minimum(wave, length - wave)
    sine = np.sin(np.pi * np.maximum(folded, 1) / length)
    cuts = np.asarray(cuts)[:, None]
    gain = np.where(folded[None] <= cuts, 1.0, (np.sin(np.pi * cuts / length) / sine[None]) ** 2)
    return np.fft.ifft(gain, axis=1).real


def hankel(line, segment, distance):
    first = segment * distance - (segment - 1)
    wrapped = np.take(line, np.arange(first, first + 2 * segment - 1), mode="wrap")
    return np.lib.stride_tricks.sliding_window_view(wrapped, segment)


def envelope_shapes(length, segment, top):
    spot = np.arange(segment)
    family = [(a / (spot + a)) ** p for a in np.geomspace(0.3, 2 * segment, 40) for p in (1, 2, 3)]
    unit = 2.0 * spot / (segment - 1) - 1.0
    family += [np.polynomial.chebyshev.chebval(unit, [0] * j + [1]) for j in range(8)]
    left, size, _ = np.linalg.svd(np.array(family).T, full_matrices=False)
    left = left[:, size > 1e-6 * size[0]]
    cuts = np.unique(np.round(np.geomspace(1, top, 40)).astype(int))
    parts = []
    for cut, line in zip(cuts, filter_lines(cuts, length)):
        turn = 2.0 * np.pi * cut / length * spot[:, None]
        both = np.concatenate([left * np.cos(turn), left * np.sin(turn)], axis=1)
        u, s, vt = np.linalg.svd(both, full_matrices=False)
        keep = s > 1e-5 * s[0]
        inverse = (vt[keep].T / s[keep]) @ u[:, keep].T
        for distance in range(1, min(length // segment // 2, 4) + 1):
            u, s, _ = np.linalg.svd(inverse @ hankel(line, segment, distance), full_matrices=False)
            scaled = (u * s)[:, s > 1e-7]
            parts += [scaled[: left.shape[1]], scaled[left.shape[1] :]]
    u, _, _ = np.linalg.svd(np.concatenate(parts, axis=1), full_matrices=False)
    shapes = left @ u[:, :SHAPES]
    return np.pad(shapes, ((0, 0), (0, SHAPES - shapes.shape[1])))


@functools.lru_cache(maxsize=None)
def filter_tables(length, segment, top):
    shapes = envelope_shapes(length, segment, top)
    spot = np.arange(segment)
    cuts = np.arange(1, top + 1)
    lines = filter_lines(cuts, length)
    half = length // segment // 2
    ranks = [NEAR_RANK] + [FAR_RANK] * (half - 1)
    mixing = np.zeros((-(-(top + 1) // PER_TILE), sum(ranks), LANES))
    for cut, line in zip(cuts, lines):
        turn = 2.0 * np.pi * ((cut * spot) % length)[:, None] / length
        both = np.concatenate([shapes * np.cos(turn), shapes * np.sin(turn)], axis=1)
        u, s, vt = np.linalg.svd(both, full_matrices=False)
        keep = s > 3e-4 * s[0]
        u, back = u[:, keep], vt[keep].T / s[keep]
        at, start = (cut % PER_TILE) * SLOT, 0
        for distance, rank in enumerate(ranks, 1):
            inner = u.T @ (hankel(line, segment, distance) @ u)
            size, vectors = np.linalg.eigh((inner + inner.T) / 2.0)
            order = np.argsort(-np.abs(size), kind="stable")[:rank]
            count = len(order)
            weights = (back @ vectors[:, order]).T
            here = mixing[cut // PER_TILE, start : start + count, at : at + SLOT]
            here[:, :SHAPES] = weights[:, :SHAPES]
            here[:, SHAPES + 1 : 2 * SHAPES + 1] = weights[:, SHAPES:]
            here[:, SHAPES] = size[order]
            start += rank
    padded = -(-segment // LANES) * LANES
    away = np.abs(np.arange(2 * padded) - (padded - 1))
    tiles = -(-2 * padded // LANES // 8) * 8
    mirrored = np.zeros((mixing.shape[0] * PER_TILE, tiles * LANES))
    mirrored[1 : top + 1, : 2 * padded] = lines[:, away]
    mirrored = mirrored.reshape(-1, tiles, LANES)
    banks = np.zeros((2, SHAPES + 1, padded))
    banks[0, :SHAPES, :segment] = shapes.T
    banks[1, :SHAPES, :segment] = shapes[::-1].T
    return mirrored.astype(np.float32), mixing.astype(np.float32), banks.astype(np.float32), ranks


def split(a):
    hi = a.astype(jnp.bfloat16)
    lo = (a - hi.astype(jnp.float32)).astype(jnp.bfloat16)
    return hi, lo


def polar_row(band, bands, rows, i):
    total = rows * bands
    return jnp.abs(2 * (band * rows + i) + 1 - total) * 5 > 2 * total


class Layout:
    def __init__(self, rows, segment, channels, ring, ranks):
        self.rows, self.segment, self.channels, self.ring = rows, segment, channels, ring
        self.padded = -(-segment // LANES) * LANES
        self.half = ring // 2
        self.tall = -(-segment // 16) * 16
        self.ranks = ranks
        self.count = sum(ranks)
        starts = np.concatenate([[0], np.cumsum(ranks)]).astype(int)
        plus = [(d, self.count + starts[d - 1], starts[d - 1], ranks[d - 1]) for d in range(1, self.half + 1)]
        minus = [(ring - d, starts[d - 1], self.count + starts[d - 1], ranks[d - 1]) for d in range(1, self.half)]
        self.peers, at = [], 0
        for step, send_row, come_row, rank in plus + minus:
            self.peers.append((step, int(send_row), int(come_row), rank, at))
            at += rank * rows
        self.total = at


def three(a):
    hi = a.astype(jnp.bfloat16)
    rest = a - hi.astype(jnp.float32)
    mid = rest.astype(jnp.bfloat16)
    return hi, mid, (rest - mid.astype(jnp.float32)).astype(jnp.bfloat16)


def filter_kernel(lay, bands, top, cut_hbm, x_hbm, line_hbm, mix_hbm, bank_hbm, y_ref, cut_ref, x_ref, line_ref, mix_ref, bank_ref, come_ref, m_ref, send, xs, left, turns, load_sem, x_sem, send_sem, recv_sem):
    seg, pad, ring, pairs = lay.segment, lay.padded, lay.ring, lay.rows // 2
    length = seg * ring
    band, me = lax.axis_index("lat"), lax.axis_index("lon")
    barrier = pltpu.get_barrier_semaphore()

    def push(n, p):
        step, _, _, rank, at = lay.peers[n]
        rows = pl.ds(pl.multiple_of(at + 2 * rank * p, 8), 2 * rank)
        return pltpu.make_async_remote_copy(
            src_ref=send.at[rows],
            dst_ref=come_ref.at[rows],
            send_sem=send_sem.at[n, p],
            recv_sem=recv_sem.at[n, p],
            device_id={"lon": lax.rem(me + step, ring)},
            device_id_type=MESH,
        )

    def fetch(p):
        return pltpu.make_async_copy(x_hbm.at[pl.ds(2 * p, 2)], x_ref.at[pl.ds(2 * p, 2)], x_sem.at[p])

    loads = [
        pltpu.make_async_copy(a, b, load_sem.at[k])
        for k, (a, b) in enumerate(((cut_hbm, cut_ref), (bank_hbm, bank_ref), (mix_hbm, mix_ref), (line_hbm, line_ref)))
    ]
    for copy in loads[:3]:
        copy.start()
    for p in range(pairs):
        fetch(p).start()
    loads[3].start()
    for step in range(1, ring):
        pl.semaphore_signal(barrier, inc=1, device_id={"lon": lax.rem(me + step, ring)}, device_id_type=MESH)

    if pad != seg:
        for r in range(lay.rows):
            for k in range(3):
                xs[r, k * pad + seg : (k + 1) * pad] = jnp.zeros((pad - seg, lay.channels), jnp.bfloat16)
    loads[0].wait()
    row = lax.broadcasted_iota(jnp.int32, (lay.rows, pad), 0)
    spot = lax.broadcasted_iota(jnp.int32, (lay.rows, pad), 1).astype(jnp.float32)
    cut = jnp.zeros((lay.rows, pad), jnp.float32)
    for i in range(lay.rows):
        cut = jnp.where(row == i, jnp.clip(cut_ref[i], 1, top).astype(jnp.float32), cut)
    for f, place in enumerate((spot, (seg - 1.0) - spot)):
        turn = cut * place
        turn = turn - jnp.floor(turn * (1.0 / length)) * length
        angle = turn * (2.0 * np.pi / length)
        turns[2 * f] = jnp.cos(angle)
        turns[2 * f + 1] = jnp.sin(angle)
    slot = lax.broadcasted_iota(jnp.int32, (lay.count, LANES), 1)
    loads[1].wait()
    loads[2].wait()

    def project(i):
        x = x_ref[i]
        hi, lo = split(x)
        xs[i, 0:seg] = hi
        xs[i, pad : pad + seg] = hi
        xs[i, 2 * pad : 2 * pad + seg] = lo
        basis = []
        for f in range(2):
            basis.append(jnp.concatenate([bank_ref[f] * turns[2 * f + w, pl.ds(i, 1), :] for w in range(2)], axis=0))
        hi, mid, lo = three(jnp.concatenate(basis, axis=1))
        right = jnp.concatenate([hi, mid, lo, hi, mid, hi], axis=0)
        cut = jnp.clip(cut_ref[i], 1, top)
        mix = jnp.where(slot // SLOT == lax.rem(cut, PER_TILE), mix_ref[cut // PER_TILE], 0.0)
        size = jnp.sum(jnp.where(lax.rem(slot, SLOT) == SHAPES, mix, 0.0), axis=1, keepdims=True)
        mix = functools.reduce(jnp.add, [mix[:, k * SLOT : (k + 1) * SLOT] for k in range(PER_TILE)])
        hi, mid, lo = three(mix)
        q = jnp.dot(jnp.concatenate([hi, hi, hi, mid, mid, lo], axis=1), right, preferred_element_type=jnp.float32)
        hi, lo = split(jnp.concatenate([q[:, :pad], q[:, pad:] * size], axis=0))
        m = jnp.concatenate([hi, lo, hi], axis=1)
        m_ref[i] = m
        return jnp.dot(m, xs[i], preferred_element_type=jnp.float32)

    def diagonal(i, s):
        line = line_ref[jnp.clip(cut_ref[i], 1, top)]
        line = jnp.concatenate([jnp.broadcast_to(line[k : k + 1], (LANES, LANES)) for k in range(2 * pad // LANES)], axis=1)
        sheet = pltpu.roll(line, 2 * pad - (LANES - 1), 1, stride=1, stride_axis=0)[:, : 2 * pad - LANES]
        hi, lo = split(sheet)
        for q in range(pad // LANES):
            cols = slice(pad - LANES * (q + 1), 2 * pad - LANES * (q + 1))
            rows = min(LANES, lay.tall - q * LANES)
            block = slice(q * LANES, q * LANES + rows)
            left[s, block, 0:pad] = hi[:rows, cols]
            left[s, block, pad : 2 * pad] = lo[:rows, cols]
            left[s, block, 2 * pad : 3 * pad] = hi[:rows, cols]
        y = jnp.dot(left[s], xs[i], preferred_element_type=jnp.float32)[:seg]
        y_ref[i] = y

    def finish(i, r, come):
        parts = [None] * (2 * lay.count)
        for (_, _, at_row, rank, _), both in zip(lay.peers, come):
            parts[at_row] = both[r * rank : (r + 1) * rank]
        unused = lay.count + sum(lay.ranks[:-1])
        parts[unused] = jnp.zeros((lay.ranks[-1], lay.channels), jnp.float32)
        hi, lo = split(jnp.concatenate([v for v in parts if v is not None], axis=0))
        right = jnp.concatenate([hi, hi, lo], axis=0)
        wide = jnp.concatenate([m_ref[i, :, k * pad : (k + 1) * pad] for k in range(3)], axis=0)
        far = lax.dot_general(wide, right, (((0,), (0,)), ((), ())), preferred_element_type=jnp.float32)[:seg]
        y_ref[i] = jnp.where(polar_row(band, bands, lay.rows, i), y_ref[i] + far, x_ref[i])

    @pl.loop(0, pairs)
    def _(p):
        fetch(p).wait()
        first, second = project(2 * p), project(2 * p + 1)
        for _, at_row, _, rank, at in lay.peers:
            both = jnp.concatenate([first[at_row : at_row + rank], second[at_row : at_row + rank]], axis=0)
            send[pl.ds(pl.multiple_of(at + 2 * rank * p, 8), 2 * rank), :] = both

        @pl.when(p == 0)
        def _():
            pl.semaphore_wait(barrier, ring - 1)

        for n in range(ring - 1):
            push(n, p).start()

    loads[3].wait()

    @pl.loop(0, pairs)
    def _(p):
        diagonal(2 * p, 0)
        diagonal(2 * p + 1, 1)

    @pl.loop(0, pairs)
    def _(p):
        for n in range(ring - 1):
            push(n, p).wait()
        come = [come_ref[pl.ds(pl.multiple_of(at + 2 * rank * p, 8), 2 * rank), :] for _, _, _, rank, at in lay.peers]
        finish(2 * p, 0, come)
        finish(2 * p + 1, 1, come)


def local(ring, bands, fields, cutoff):
    rows, segment, channels = fields.shape
    length, total = ring * segment, rows * bands
    row_ids = np.arange(total)
    polar = np.abs(2 * row_ids + 1 - total) * 5 > 2 * total
    poles = np.minimum(row_ids, total - 1 - row_ids)
    top = int(1 + (length // 2 - 1) * (2 * poles[polar].max() + 1) // total)
    lines, mixing, bank, ranks = filter_tables(length, segment, top)
    lay = Layout(rows, segment, channels, ring, ranks)
    pad = lay.padded
    f32, bf16 = jnp.float32, jnp.bfloat16
    hbm = pl.BlockSpec(memory_space=pltpu.HBM)
    inputs = [pltpu.with_memory_space_constraint(a, pltpu.HBM) for a in (cutoff, fields, *map(jnp.asarray, (lines, mixing, bank)))]
    return pl.pallas_call(
        functools.partial(filter_kernel, lay, bands, top),
        out_shape=jax.ShapeDtypeStruct(fields.shape, fields.dtype),
        in_specs=[hbm] * 5,
        out_specs=pl.BlockSpec(memory_space=pltpu.VMEM),
        scratch_shapes=[
            pltpu.SMEM((rows,), jnp.int32),
            pltpu.VMEM(fields.shape, f32),
            pltpu.VMEM(lines.shape, f32),
            pltpu.VMEM(mixing.shape, f32),
            pltpu.VMEM(bank.shape, f32),
            pltpu.VMEM((lay.total, channels), f32),
            pltpu.VMEM((rows, 2 * lay.count, 3 * pad), bf16),
            pltpu.VMEM((lay.total, channels), f32),
            pltpu.VMEM((rows, 3 * pad, channels), bf16),
            pltpu.VMEM((2, lay.tall, 3 * pad), bf16),
            pltpu.VMEM((4, rows, pad), f32),
            pltpu.SemaphoreType.DMA((4,)),
            pltpu.SemaphoreType.DMA((rows // 2,)),
            pltpu.SemaphoreType.DMA((ring - 1, rows // 2)),
            pltpu.SemaphoreType.DMA((ring - 1, rows // 2)),
        ],
        compiler_params=pltpu.CompilerParams(collective_id=0, has_side_effects=True, vmem_limit_bytes=48 * 1024 * 1024),
        name="filter",
    )(*inputs)


def solution(mesh):
    return jax.shard_map(
        functools.partial(local, mesh.shape["lon"], mesh.shape["lat"]),
        mesh=mesh,
        in_specs=(P("lat", "lon", None), P("lat")),
        out_specs=P("lat", "lon", None),
        check_vma=False,
    )
```

```python
import functools

import jax
import jax.numpy as jnp
import numpy as np
from jax import lax
from jax.experimental import pallas as pl
from jax.experimental.pallas import tpu as pltpu
from jax.sharding import PartitionSpec as P

LANES = 128
SHAPES = 15
SLOT = 2 * SHAPES + 2
PER_TILE = LANES // SLOT
NEAR_RANK, FAR_RANK = 12, 4
MESH = pl.DeviceIdType.MESH


def filter_lines(cuts, length):
    wave = np.arange(length)
    folded = np.minimum(wave, length - wave)
    sine = np.sin(np.pi * np.maximum(folded, 1) / length)
    cuts = np.asarray(cuts)[:, None]
    gain = np.where(folded[None] <= cuts, 1.0, (np.sin(np.pi * cuts / length) / sine[None]) ** 2)
    return np.fft.ifft(gain, axis=1).real


def hankel(line, segment, distance):
    first = segment * distance - (segment - 1)
    wrapped = np.take(line, np.arange(first, first + 2 * segment - 1), mode="wrap")
    return np.lib.stride_tricks.sliding_window_view(wrapped, segment)


def envelope_shapes(length, segment, top):
    spot = np.arange(segment)
    family = [(a / (spot + a)) ** p for a in np.geomspace(0.3, 2 * segment, 40) for p in (1, 2, 3)]
    unit = 2.0 * spot / (segment - 1) - 1.0
    family += [np.polynomial.chebyshev.chebval(unit, [0] * j + [1]) for j in range(8)]
    left, size, _ = np.linalg.svd(np.array(family).T, full_matrices=False)
    left = left[:, size > 1e-6 * size[0]]
    cuts = np.unique(np.round(np.geomspace(1, top, 40)).astype(int))
    parts = []
    for cut, line in zip(cuts, filter_lines(cuts, length)):
        turn = 2.0 * np.pi * cut / length * spot[:, None]
        both = np.concatenate([left * np.cos(turn), left * np.sin(turn)], axis=1)
        u, s, vt = np.linalg.svd(both, full_matrices=False)
        keep = s > 1e-5 * s[0]
        inverse = (vt[keep].T / s[keep]) @ u[:, keep].T
        for distance in range(1, min(length // segment // 2, 4) + 1):
            u, s, _ = np.linalg.svd(inverse @ hankel(line, segment, distance), full_matrices=False)
            scaled = (u * s)[:, s > 1e-7]
            parts += [scaled[: left.shape[1]], scaled[left.shape[1] :]]
    u, _, _ = np.linalg.svd(np.concatenate(parts, axis=1), full_matrices=False)
    shapes = left @ u[:, :SHAPES]
    return np.pad(shapes, ((0, 0), (0, SHAPES - shapes.shape[1])))


@functools.lru_cache(maxsize=None)
def filter_tables(length, segment, top):
    shapes = envelope_shapes(length, segment, top)
    spot = np.arange(segment)
    cuts = np.arange(1, top + 1)
    lines = filter_lines(cuts, length)
    half = length // segment // 2
    ranks = [NEAR_RANK] + [FAR_RANK] * (half - 1)
    mixing = np.zeros((-(-(top + 1) // PER_TILE), sum(ranks), LANES))
    for cut, line in zip(cuts, lines):
        turn = 2.0 * np.pi * ((cut * spot) % length)[:, None] / length
        both = np.concatenate([shapes * np.cos(turn), shapes * np.sin(turn)], axis=1)
        u, s, vt = np.linalg.svd(both, full_matrices=False)
        keep = s > 3e-4 * s[0]
        u, back = u[:, keep], vt[keep].T / s[keep]
        at, start = (cut % PER_TILE) * SLOT, 0
        for distance, rank in enumerate(ranks, 1):
            inner = u.T @ (hankel(line, segment, distance) @ u)
            size, vectors = np.linalg.eigh((inner + inner.T) / 2.0)
            order = np.argsort(-np.abs(size), kind="stable")[:rank]
            count = len(order)
            weights = (back @ vectors[:, order]).T
            here = mixing[cut // PER_TILE, start : start + count, at : at + SLOT]
            here[:, :SHAPES] = weights[:, :SHAPES]
            here[:, SHAPES + 1 : 2 * SHAPES + 1] = weights[:, SHAPES:]
            here[:, SHAPES] = size[order]
            start += rank
    padded = -(-segment // LANES) * LANES
    tiles = padded // LANES
    halves = np.zeros((-(-(top + 1) // 8) * 8, tiles * LANES))
    halves[1 : top + 1] = lines[:, : tiles * LANES]
    halves = halves.reshape(-1, 8 * tiles, LANES)
    banks = np.zeros((2, SHAPES + 1, padded))
    banks[0, :SHAPES, :segment] = shapes.T
    banks[1, :SHAPES, :segment] = shapes[::-1].T
    return halves.astype(np.float32), mixing.astype(np.float32), banks.astype(np.float32), ranks


def split(a):
    hi = a.astype(jnp.bfloat16)
    lo = (a - hi.astype(jnp.float32)).astype(jnp.bfloat16)
    return hi, lo


def polar_row(band, bands, rows, i):
    total = rows * bands
    return jnp.abs(2 * (band * rows + i) + 1 - total) * 5 > 2 * total


class Layout:
    def __init__(self, rows, segment, channels, ring, ranks):
        self.rows, self.segment, self.channels, self.ring = rows, segment, channels, ring
        self.padded = -(-segment // LANES) * LANES
        self.half = ring // 2
        self.tall = -(-segment // 16) * 16
        self.ranks = ranks
        self.count = sum(ranks)
        starts = np.concatenate([[0], np.cumsum(ranks)]).astype(int)
        plus = [(d, self.count + starts[d - 1], starts[d - 1], ranks[d - 1]) for d in range(1, self.half + 1)]
        minus = [(ring - d, starts[d - 1], self.count + starts[d - 1], ranks[d - 1]) for d in range(1, self.half)]
        self.peers, at = [], 0
        for step, send_row, come_row, rank in plus + minus:
            self.peers.append((step, int(send_row), int(come_row), rank, at))
            at += rank * rows
        self.total = at


def three(a):
    hi = a.astype(jnp.bfloat16)
    rest = a - hi.astype(jnp.float32)
    mid = rest.astype(jnp.bfloat16)
    return hi, mid, (rest - mid.astype(jnp.float32)).astype(jnp.bfloat16)


def filter_kernel(lay, bands, top, cut_hbm, x_hbm, line_hbm, mix_hbm, bank_hbm, y_ref, cut_ref, x_ref, line_ref, mix_ref, bank_ref, come_ref, m_ref, send, xs, left, turns, both, load_sem, x_sem, send_sem, recv_sem):
    seg, pad, ring, pairs = lay.segment, lay.padded, lay.ring, lay.rows // 2
    length, tops = seg * ring, 2 * lay.count
    band, me = lax.axis_index("lat"), lax.axis_index("lon")
    barrier = pltpu.get_barrier_semaphore()

    def push(n, p):
        step, _, _, rank, at = lay.peers[n]
        rows = pl.ds(pl.multiple_of(at + 2 * rank * p, 8), 2 * rank)
        return pltpu.make_async_remote_copy(
            src_ref=send.at[rows],
            dst_ref=come_ref.at[rows],
            send_sem=send_sem.at[n, p],
            recv_sem=recv_sem.at[n, p],
            device_id={"lon": lax.rem(me + step, ring)},
            device_id_type=MESH,
        )

    def fetch(p):
        return pltpu.make_async_copy(x_hbm.at[pl.ds(2 * p, 2)], x_ref.at[pl.ds(2 * p, 2)], x_sem.at[p])

    loads = [
        pltpu.make_async_copy(a, b, load_sem.at[k])
        for k, (a, b) in enumerate(((cut_hbm, cut_ref), (bank_hbm, bank_ref), (mix_hbm, mix_ref), (line_hbm, line_ref)))
    ]
    for copy in loads[:3]:
        copy.start()
    fetch(0).start()
    for step in range(1, ring):
        pl.semaphore_signal(barrier, inc=1, device_id={"lon": lax.rem(me + step, ring)}, device_id_type=MESH)

    if pad != seg:
        for r in range(lay.rows):
            for k in range(3):
                xs[r, k * pad + seg : (k + 1) * pad] = jnp.zeros((pad - seg, lay.channels), jnp.bfloat16)
    loads[0].wait()
    row = lax.broadcasted_iota(jnp.int32, (lay.rows, pad), 0)
    spot = lax.broadcasted_iota(jnp.int32, (lay.rows, pad), 1).astype(jnp.float32)
    cut = jnp.zeros((lay.rows, pad), jnp.float32)
    for i in range(lay.rows):
        cut = jnp.where(row == i, jnp.clip(cut_ref[i], 1, top).astype(jnp.float32), cut)
    for f, place in enumerate((spot, (seg - 1.0) - spot)):
        turn = cut * place
        turn = turn - jnp.floor(turn * (1.0 / length)) * length
        angle = turn * (2.0 * np.pi / length)
        turns[2 * f] = jnp.cos(angle)
        turns[2 * f + 1] = jnp.sin(angle)
    slot = lax.broadcasted_iota(jnp.int32, (lay.count, LANES), 1)
    loads[1].wait()
    loads[2].wait()
    for copy in [fetch(1), loads[3]] + [fetch(p) for p in range(2, pairs)]:
        copy.start()

    def mixed(i):
        x = x_ref[i]
        hi, lo = split(x)
        xs[i, 0:seg] = hi
        xs[i, pad : pad + seg] = hi
        xs[i, 2 * pad : 2 * pad + seg] = lo
        basis = []
        for f in range(2):
            basis.append(jnp.concatenate([bank_ref[f] * turns[2 * f + w, pl.ds(i, 1), :] for w in range(2)], axis=0))
        hi, mid, lo = three(jnp.concatenate(basis, axis=1))
        right = jnp.concatenate([hi, mid, lo, hi, mid, hi], axis=0)
        cut = jnp.clip(cut_ref[i], 1, top)
        mix = jnp.where(slot // SLOT == lax.rem(cut, PER_TILE), mix_ref[cut // PER_TILE], 0.0)
        size = jnp.sum(jnp.where(lax.rem(slot, SLOT) == SHAPES, mix, 0.0), axis=1, keepdims=True)
        mix = functools.reduce(jnp.add, [mix[:, k * SLOT : (k + 1) * SLOT] for k in range(PER_TILE)])
        hi, mid, lo = three(mix)
        q = jnp.dot(jnp.concatenate([hi, hi, hi, mid, mid, lo], axis=1), right, preferred_element_type=jnp.float32)
        hi, lo = split(jnp.concatenate([q[:, :pad], q[:, pad:] * size], axis=0))
        m = jnp.concatenate([hi, lo, hi], axis=1)
        m_ref[i] = m
        return m

    def mirror():
        tiles = pad // LANES
        rows = []
        for i in range(lay.rows):
            cut = jnp.clip(cut_ref[i], 1, top)
            rows += [line_ref[cut // 8, pl.ds(lax.rem(cut, 8) * tiles + k, 1), :] for k in range(tiles)]
        ahead = jnp.concatenate(rows, axis=0)
        count = ahead.shape[0]
        lane = lax.broadcasted_iota(jnp.int32, (LANES, LANES), 0) + lax.broadcasted_iota(jnp.int32, (LANES, LANES), 1)
        turn = (lane == LANES).astype(jnp.bfloat16)
        back = jnp.dot(jnp.concatenate(three(ahead), axis=0), turn, preferred_element_type=jnp.float32)
        back = back[:count] + back[count : 2 * count] + back[2 * count :]
        ahead_next = jnp.concatenate([ahead[1:], ahead[:1]], axis=0)
        back = jnp.where(lax.broadcasted_iota(jnp.int32, back.shape, 1) == 0, ahead_next, back)
        for i in range(lay.rows):
            for k in range(tiles):
                at = i * tiles + k
                both[pl.ds(i, 1), (tiles - 1 - k) * LANES : (tiles - k) * LANES] = back[at : at + 1]
                both[pl.ds(i, 1), (tiles + k) * LANES : (tiles + k + 1) * LANES] = ahead[at : at + 1]

    def toeplitz(i, s):
        line = jnp.broadcast_to(both[pl.ds(i, 1), :], (LANES, 2 * pad))
        sheet = pltpu.roll(line, 2 * pad - LANES, 1, stride=1, stride_axis=0)[:, : 2 * pad - LANES]
        hi, lo = split(sheet)
        for q in range(pad // LANES):
            cols = slice(pad - LANES * (q + 1), 2 * pad - LANES * (q + 1))
            rows = min(LANES, lay.tall - q * LANES)
            block = slice(tops + q * LANES, tops + q * LANES + rows)
            left[s, block, 0:pad] = hi[:rows, cols]
            left[s, block, pad : 2 * pad] = lo[:rows, cols]
            left[s, block, 2 * pad : 3 * pad] = hi[:rows, cols]

    def keep(i, y):
        on = polar_row(band, bands, lay.rows, i)

        @pl.when(on)
        def _():
            y_ref[i] = y

        @pl.when(jnp.logical_not(on))
        def _():
            y_ref[i] = x_ref[i]

    def stacked(i, s):
        left[s, 0:tops] = mixed(i)
        toeplitz(i, s)
        y = jnp.dot(left[s], xs[i], preferred_element_type=jnp.float32)
        keep(i, y[tops : tops + seg])
        return y[:tops]

    def post(p, first, second):
        for _, at_row, _, rank, at in lay.peers:
            two = jnp.concatenate([first[at_row : at_row + rank], second[at_row : at_row + rank]], axis=0)
            send[pl.ds(pl.multiple_of(at + 2 * rank * p, 8), 2 * rank), :] = two

    def finish(i, r, come):
        parts = [None] * (2 * lay.count)
        for (_, _, at_row, rank, _), both in zip(lay.peers, come):
            parts[at_row] = both[r * rank : (r + 1) * rank]
        unused = lay.count + sum(lay.ranks[:-1])
        parts[unused] = jnp.zeros((lay.ranks[-1], lay.channels), jnp.float32)
        hi, lo = split(jnp.concatenate([v for v in parts if v is not None], axis=0))
        right = jnp.concatenate([hi, hi, lo], axis=0)
        wide = jnp.concatenate([m_ref[i, :, k * pad : (k + 1) * pad] for k in range(3)], axis=0)
        far = lax.dot_general(wide, right, (((0,), (0,)), ((), ())), preferred_element_type=jnp.float32)[:seg]

        @pl.when(polar_row(band, bands, lay.rows, i))
        def _():
            y_ref[i] += far

    fetch(0).wait()
    post(0, *[jnp.dot(mixed(i), xs[i], preferred_element_type=jnp.float32) for i in range(2)])
    pl.semaphore_wait(barrier, ring - 1)
    for n in range(ring - 1):
        push(n, 0).start()
    loads[3].wait()
    mirror()

    @pl.loop(1, pairs)
    def _(p):
        fetch(p).wait()
        post(p, stacked(2 * p, 0), stacked(2 * p + 1, 1))
        for n in range(ring - 1):
            push(n, p).start()

    for i in range(2):
        toeplitz(i, i)
        keep(i, jnp.dot(left[i, tops:], xs[i], preferred_element_type=jnp.float32)[:seg])

    @pl.loop(0, pairs)
    def _(p):
        for n in range(ring - 1):
            push(n, p).wait()
        come = [come_ref[pl.ds(pl.multiple_of(at + 2 * rank * p, 8), 2 * rank), :] for _, _, _, rank, at in lay.peers]
        finish(2 * p, 0, come)
        finish(2 * p + 1, 1, come)


def local(ring, bands, fields, cutoff):
    rows, segment, channels = fields.shape
    length, total = ring * segment, rows * bands
    row_ids = np.arange(total)
    polar = np.abs(2 * row_ids + 1 - total) * 5 > 2 * total
    poles = np.minimum(row_ids, total - 1 - row_ids)
    top = int(1 + (length // 2 - 1) * (2 * poles[polar].max() + 1) // total)
    lines, mixing, bank, ranks = filter_tables(length, segment, top)
    lay = Layout(rows, segment, channels, ring, ranks)
    pad = lay.padded
    f32, bf16 = jnp.float32, jnp.bfloat16
    hbm = pl.BlockSpec(memory_space=pltpu.HBM)
    inputs = [pltpu.with_memory_space_constraint(a, pltpu.HBM) for a in (cutoff, fields, *map(jnp.asarray, (lines, mixing, bank)))]
    return pl.pallas_call(
        functools.partial(filter_kernel, lay, bands, top),
        out_shape=jax.ShapeDtypeStruct(fields.shape, fields.dtype),
        in_specs=[hbm] * 5,
        out_specs=pl.BlockSpec(memory_space=pltpu.VMEM),
        scratch_shapes=[
            pltpu.SMEM((rows,), jnp.int32),
            pltpu.VMEM(fields.shape, f32),
            pltpu.VMEM(lines.shape, f32),
            pltpu.VMEM(mixing.shape, f32),
            pltpu.VMEM(bank.shape, f32),
            pltpu.VMEM((lay.total, channels), f32),
            pltpu.VMEM((rows, 2 * lay.count, 3 * pad), bf16),
            pltpu.VMEM((lay.total, channels), f32),
            pltpu.VMEM((rows, 3 * pad, channels), bf16),
            pltpu.VMEM((2, -(-2 * lay.count // 16) * 16 + lay.tall, 3 * pad), bf16),
            pltpu.VMEM((4, rows, pad), f32),
            pltpu.VMEM((rows, 2 * pad), f32),
            pltpu.SemaphoreType.DMA((4,)),
            pltpu.SemaphoreType.DMA((rows // 2,)),
            pltpu.SemaphoreType.DMA((ring - 1, rows // 2)),
            pltpu.SemaphoreType.DMA((ring - 1, rows // 2)),
        ],
        compiler_params=pltpu.CompilerParams(collective_id=0, has_side_effects=True, vmem_limit_bytes=48 * 1024 * 1024),
        name="filter",
    )(*inputs)


def solution(mesh):
    return jax.shard_map(
        functools.partial(local, mesh.shape["lon"], mesh.shape["lat"]),
        mesh=mesh,
        in_specs=(P("lat", "lon", None), P("lat")),
        out_specs=P("lat", "lon", None),
        check_vma=False,
    )
```

```python
import functools

import jax
import jax.numpy as jnp
import numpy as np
from jax import lax
from jax.experimental import pallas as pl
from jax.experimental.pallas import tpu as pltpu
from jax.sharding import PartitionSpec as P

LANES = 128
SHAPES = 15
SLOT = 2 * SHAPES + 2
PER_TILE = LANES // SLOT
NEAR_RANK, FAR_RANK = 12, 4
MESH = pl.DeviceIdType.MESH


def filter_lines(cuts, length):
    wave = np.arange(length)
    folded = np.minimum(wave, length - wave)
    sine = np.sin(np.pi * np.maximum(folded, 1) / length)
    cuts = np.asarray(cuts)[:, None]
    gain = np.where(folded[None] <= cuts, 1.0, (np.sin(np.pi * cuts / length) / sine[None]) ** 2)
    return np.fft.ifft(gain, axis=1).real


def hankel(line, segment, distance):
    first = segment * distance - (segment - 1)
    wrapped = np.take(line, np.arange(first, first + 2 * segment - 1), mode="wrap")
    return np.lib.stride_tricks.sliding_window_view(wrapped, segment)


def envelope_shapes(length, segment, top):
    spot = np.arange(segment)
    family = [(a / (spot + a)) ** p for a in np.geomspace(0.3, 2 * segment, 40) for p in (1, 2, 3)]
    unit = 2.0 * spot / (segment - 1) - 1.0
    family += [np.polynomial.chebyshev.chebval(unit, [0] * j + [1]) for j in range(8)]
    left, size, _ = np.linalg.svd(np.array(family).T, full_matrices=False)
    left = left[:, size > 1e-6 * size[0]]
    cuts = np.unique(np.round(np.geomspace(1, top, 40)).astype(int))
    parts = []
    for cut, line in zip(cuts, filter_lines(cuts, length)):
        turn = 2.0 * np.pi * cut / length * spot[:, None]
        both = np.concatenate([left * np.cos(turn), left * np.sin(turn)], axis=1)
        u, s, vt = np.linalg.svd(both, full_matrices=False)
        keep = s > 1e-5 * s[0]
        inverse = (vt[keep].T / s[keep]) @ u[:, keep].T
        for distance in range(1, min(length // segment // 2, 4) + 1):
            u, s, _ = np.linalg.svd(inverse @ hankel(line, segment, distance), full_matrices=False)
            scaled = (u * s)[:, s > 1e-7]
            parts += [scaled[: left.shape[1]], scaled[left.shape[1] :]]
    u, _, _ = np.linalg.svd(np.concatenate(parts, axis=1), full_matrices=False)
    shapes = left @ u[:, :SHAPES]
    return np.pad(shapes, ((0, 0), (0, SHAPES - shapes.shape[1])))


@functools.lru_cache(maxsize=None)
def filter_tables(length, segment, top):
    shapes = envelope_shapes(length, segment, top)
    spot = np.arange(segment)
    cuts = np.arange(1, top + 1)
    lines = filter_lines(cuts, length)
    half = length // segment // 2
    ranks = [NEAR_RANK] + [FAR_RANK] * (half - 1)
    mixing = np.zeros((-(-(top + 1) // PER_TILE), sum(ranks), LANES))
    for cut, line in zip(cuts, lines):
        turn = 2.0 * np.pi * ((cut * spot) % length)[:, None] / length
        both = np.concatenate([shapes * np.cos(turn), shapes * np.sin(turn)], axis=1)
        u, s, vt = np.linalg.svd(both, full_matrices=False)
        keep = s > 3e-4 * s[0]
        u, back = u[:, keep], vt[keep].T / s[keep]
        at, start = (cut % PER_TILE) * SLOT, 0
        for distance, rank in enumerate(ranks, 1):
            inner = u.T @ (hankel(line, segment, distance) @ u)
            size, vectors = np.linalg.eigh((inner + inner.T) / 2.0)
            order = np.argsort(-np.abs(size), kind="stable")[:rank]
            count = len(order)
            weights = (back @ vectors[:, order]).T
            here = mixing[cut // PER_TILE, start : start + count, at : at + SLOT]
            here[:, :SHAPES] = weights[:, :SHAPES]
            here[:, SHAPES + 1 : 2 * SHAPES + 1] = weights[:, SHAPES:]
            here[:, SHAPES] = size[order]
            start += rank
    padded = -(-segment // LANES) * LANES
    tiles = padded // LANES
    halves = np.zeros((-(-(top + 1) // 8) * 8, tiles * LANES))
    halves[1 : top + 1] = lines[:, : tiles * LANES]
    halves = halves.reshape(-1, 8 * tiles, LANES)
    banks = np.zeros((2, SHAPES + 1, padded))
    banks[0, :SHAPES, :segment] = shapes.T
    banks[1, :SHAPES, :segment] = shapes[::-1].T
    return halves.astype(np.float32), mixing.astype(np.float32), banks.astype(np.float32), ranks


def split(a):
    hi = a.astype(jnp.bfloat16)
    lo = (a - hi.astype(jnp.float32)).astype(jnp.bfloat16)
    return hi, lo


def polar_row(band, bands, rows, i):
    total = rows * bands
    return jnp.abs(2 * (band * rows + i) + 1 - total) * 5 > 2 * total


class Layout:
    def __init__(self, rows, segment, channels, ring, ranks):
        self.rows, self.segment, self.channels, self.ring = rows, segment, channels, ring
        self.padded = -(-segment // LANES) * LANES
        self.half = ring // 2
        self.tall = -(-segment // 16) * 16
        self.ranks = ranks
        self.count = sum(ranks)
        starts = np.concatenate([[0], np.cumsum(ranks)]).astype(int)
        plus = [(d, self.count + starts[d - 1], starts[d - 1], ranks[d - 1]) for d in range(1, self.half + 1)]
        minus = [(ring - d, starts[d - 1], self.count + starts[d - 1], ranks[d - 1]) for d in range(1, self.half)]
        self.peers, at = [], 0
        for step, send_row, come_row, rank in plus + minus:
            self.peers.append((step, int(send_row), int(come_row), rank, at))
            at += rank * rows
        self.total = at


def three(a):
    hi = a.astype(jnp.bfloat16)
    rest = a - hi.astype(jnp.float32)
    mid = rest.astype(jnp.bfloat16)
    return hi, mid, (rest - mid.astype(jnp.float32)).astype(jnp.bfloat16)


def filter_kernel(lay, bands, top, cut_hbm, x_hbm, line_hbm, mix_hbm, bank_hbm, y_ref, cut_ref, x_ref, line_ref, mix_ref, bank_ref, come_ref, m_ref, send, xs, left, turns, both, load_sem, x_sem, send_sem, recv_sem):
    seg, pad, ring, pairs = lay.segment, lay.padded, lay.ring, lay.rows // 2
    length = seg * ring
    band, me = lax.axis_index("lat"), lax.axis_index("lon")
    barrier = pltpu.get_barrier_semaphore()
    total = lay.rows * bands
    polar = [abs(2 * i + 1 - total) * 5 > 2 * total for i in range(total)]
    mixed_pairs = polar[0::2] != polar[1::2]

    def push(n, p):
        step, _, _, rank, at = lay.peers[n]
        rows = pl.ds(pl.multiple_of(at + 2 * rank * p, 8), 2 * rank)
        return pltpu.make_async_remote_copy(
            src_ref=send.at[rows],
            dst_ref=come_ref.at[rows],
            send_sem=send_sem.at[n, p],
            recv_sem=recv_sem.at[n, p],
            device_id={"lon": lax.rem(me + step, ring)},
            device_id_type=MESH,
        )

    def fetch(p):
        return pltpu.make_async_copy(x_hbm.at[pl.ds(2 * p, 2)], x_ref.at[pl.ds(2 * p, 2)], x_sem.at[p])

    loads = [
        pltpu.make_async_copy(a, b, load_sem.at[k])
        for k, (a, b) in enumerate(((cut_hbm, cut_ref), (bank_hbm, bank_ref), (mix_hbm, mix_ref), (line_hbm, line_ref)))
    ]
    for copy in loads[:3]:
        copy.start()
    fetch(0).start()
    for step in range(1, ring):
        pl.semaphore_signal(barrier, inc=1, device_id={"lon": lax.rem(me + step, ring)}, device_id_type=MESH)

    if pad != seg:
        for r in range(lay.rows):
            for k in range(3):
                xs[r, k * pad + seg : (k + 1) * pad] = jnp.zeros((pad - seg, lay.channels), jnp.bfloat16)
    loads[0].wait()
    for copy in [fetch(1), loads[3]] + [fetch(p) for p in range(2, pairs)]:
        copy.start()
    row = lax.broadcasted_iota(jnp.int32, (lay.rows, pad), 0)
    spot = lax.broadcasted_iota(jnp.int32, (lay.rows, pad), 1).astype(jnp.float32)
    cut = jnp.zeros((lay.rows, pad), jnp.float32)
    for i in range(lay.rows):
        cut = jnp.where(row == i, jnp.clip(cut_ref[i], 1, top).astype(jnp.float32), cut)
    for f, place in enumerate((spot, (seg - 1.0) - spot)):
        turn = cut * place
        turn = turn - jnp.floor(turn * (1.0 / length)) * length
        angle = turn * (2.0 * np.pi / length)
        turns[2 * f] = jnp.cos(angle)
        turns[2 * f + 1] = jnp.sin(angle)
    slot = lax.broadcasted_iota(jnp.int32, (lay.count, LANES), 1)
    loads[1].wait()
    loads[2].wait()

    def mixed(i):
        x = x_ref[i]
        hi, lo = split(x)
        xs[i, 0:seg] = hi
        xs[i, pad : pad + seg] = hi
        xs[i, 2 * pad : 2 * pad + seg] = lo
        basis = []
        for f in range(2):
            basis.append(jnp.concatenate([bank_ref[f] * turns[2 * f + w, pl.ds(i, 1), :] for w in range(2)], axis=0))
        hi, mid, lo = three(jnp.concatenate(basis, axis=1))
        right = jnp.concatenate([hi, mid, lo, hi, mid, hi], axis=0)
        cut = jnp.clip(cut_ref[i], 1, top)
        mix = jnp.where(slot // SLOT == lax.rem(cut, PER_TILE), mix_ref[cut // PER_TILE], 0.0)
        size = jnp.sum(jnp.where(lax.rem(slot, SLOT) == SHAPES, mix, 0.0), axis=1, keepdims=True)
        mix = functools.reduce(jnp.add, [mix[:, k * SLOT : (k + 1) * SLOT] for k in range(PER_TILE)])
        hi, mid, lo = three(mix)
        q = jnp.dot(jnp.concatenate([hi, hi, hi, mid, mid, lo], axis=1), right, preferred_element_type=jnp.float32)
        hi, lo = split(jnp.concatenate([q[:, :pad], q[:, pad:] * size], axis=0))
        m = jnp.concatenate([hi, lo, hi], axis=1)
        m_ref[i] = m
        return m

    def mirror():
        tiles = pad // LANES
        rows = []
        for i in range(lay.rows):
            cut = jnp.clip(cut_ref[i], 1, top)
            rows += [line_ref[cut // 8, pl.ds(lax.rem(cut, 8) * tiles + k, 1), :] for k in range(tiles)]
        ahead = jnp.concatenate(rows, axis=0)
        count = ahead.shape[0]
        lane = lax.broadcasted_iota(jnp.int32, (LANES, LANES), 0) + lax.broadcasted_iota(jnp.int32, (LANES, LANES), 1)
        turn = (lane == LANES).astype(jnp.bfloat16)
        back = jnp.dot(jnp.concatenate(three(ahead), axis=0), turn, preferred_element_type=jnp.float32)
        back = back[:count] + back[count : 2 * count] + back[2 * count :]
        ahead_next = jnp.concatenate([ahead[1:], ahead[:1]], axis=0)
        back = jnp.where(lax.broadcasted_iota(jnp.int32, back.shape, 1) == 0, ahead_next, back)
        for i in range(lay.rows):
            for k in range(tiles):
                at = i * tiles + k
                both[pl.ds(i, 1), (tiles - 1 - k) * LANES : (tiles - k) * LANES] = back[at : at + 1]
                both[pl.ds(i, 1), (tiles + k) * LANES : (tiles + k + 1) * LANES] = ahead[at : at + 1]

    def toeplitz(i, s):
        line = jnp.broadcast_to(both[pl.ds(i, 1), :], (LANES, 2 * pad))
        sheet = pltpu.roll(line, 2 * pad - LANES, 1, stride=1, stride_axis=0)[:, : 2 * pad - LANES]
        hi, lo = split(sheet)
        for q in range(pad // LANES):
            cols = slice(pad - LANES * (q + 1), 2 * pad - LANES * (q + 1))
            rows = min(LANES, lay.tall - q * LANES)
            block = slice(q * LANES, q * LANES + rows)
            left[s, block, 0:pad] = hi[:rows, cols]
            left[s, block, pad : 2 * pad] = lo[:rows, cols]
            left[s, block, 2 * pad : 3 * pad] = hi[:rows, cols]

    def post(p, first, second):
        for _, at_row, _, rank, at in lay.peers:
            two = jnp.concatenate([first[at_row : at_row + rank], second[at_row : at_row + rank]], axis=0)
            send[pl.ds(pl.multiple_of(at + 2 * rank * p, 8), 2 * rank), :] = two

    def finish(i, r, come):
        parts = [None] * (2 * lay.count)
        for (_, _, at_row, rank, _), both in zip(lay.peers, come):
            parts[at_row] = both[r * rank : (r + 1) * rank]
        unused = lay.count + sum(lay.ranks[:-1])
        parts[unused] = jnp.zeros((lay.ranks[-1], lay.channels), jnp.float32)
        hi, lo = split(jnp.concatenate([v for v in parts if v is not None], axis=0))
        right = jnp.concatenate([hi, hi, lo], axis=0)
        wide = jnp.concatenate([m_ref[i, :, k * pad : (k + 1) * pad] for k in range(3)], axis=0)
        far = lax.dot_general(wide, right, (((0,), (0,)), ((), ())), preferred_element_type=jnp.float32)[:seg]
        y = y_ref[i] + far
        y_ref[i] = jnp.where(polar_row(band, bands, lay.rows, i), y, x_ref[i]) if mixed_pairs else y

    @pl.loop(0, pairs)
    def _(p):
        fetch(p).wait()
        post(p, *[jnp.dot(mixed(2 * p + r), xs[2 * p + r], preferred_element_type=jnp.float32) for r in range(2)])

        @pl.when(p == 0)
        def _():
            pl.semaphore_wait(barrier, ring - 1)

        for n in range(ring - 1):
            push(n, p).start()

    loads[3].wait()
    mirror()

    @pl.loop(0, pairs)
    def _(p):
        for r in range(2):
            toeplitz(2 * p + r, r)
            y_ref[2 * p + r] = jnp.dot(left[r], xs[2 * p + r], preferred_element_type=jnp.float32)[:seg]

    @pl.loop(0, pairs)
    def _(p):
        for n in range(ring - 1):
            push(n, p).wait()
        any_on = jnp.logical_or(polar_row(band, bands, lay.rows, 2 * p), polar_row(band, bands, lay.rows, 2 * p + 1))

        @pl.when(any_on)
        def _():
            come = [come_ref[pl.ds(pl.multiple_of(at + 2 * rank * p, 8), 2 * rank), :] for _, _, _, rank, at in lay.peers]
            finish(2 * p, 0, come)
            finish(2 * p + 1, 1, come)

        @pl.when(jnp.logical_not(any_on))
        def _():
            y_ref[pl.ds(2 * p, 2)] = x_ref[pl.ds(2 * p, 2)]


def local(ring, bands, fields, cutoff):
    rows, segment, channels = fields.shape
    length, total = ring * segment, rows * bands
    row_ids = np.arange(total)
    polar = np.abs(2 * row_ids + 1 - total) * 5 > 2 * total
    poles = np.minimum(row_ids, total - 1 - row_ids)
    top = int(1 + (length // 2 - 1) * (2 * poles[polar].max() + 1) // total)
    lines, mixing, bank, ranks = filter_tables(length, segment, top)
    lay = Layout(rows, segment, channels, ring, ranks)
    pad = lay.padded
    f32, bf16 = jnp.float32, jnp.bfloat16
    hbm = pl.BlockSpec(memory_space=pltpu.HBM)
    inputs = [pltpu.with_memory_space_constraint(a, pltpu.HBM) for a in (cutoff, fields, *map(jnp.asarray, (lines, mixing, bank)))]
    return pl.pallas_call(
        functools.partial(filter_kernel, lay, bands, top),
        out_shape=jax.ShapeDtypeStruct(fields.shape, fields.dtype),
        in_specs=[hbm] * 5,
        out_specs=pl.BlockSpec(memory_space=pltpu.VMEM),
        scratch_shapes=[
            pltpu.SMEM((rows,), jnp.int32),
            pltpu.VMEM(fields.shape, f32),
            pltpu.VMEM(lines.shape, f32),
            pltpu.VMEM(mixing.shape, f32),
            pltpu.VMEM(bank.shape, f32),
            pltpu.VMEM((lay.total, channels), f32),
            pltpu.VMEM((rows, 2 * lay.count, 3 * pad), bf16),
            pltpu.VMEM((lay.total, channels), f32),
            pltpu.VMEM((rows, 3 * pad, channels), bf16),
            pltpu.VMEM((2, lay.tall, 3 * pad), bf16),
            pltpu.VMEM((4, rows, pad), f32),
            pltpu.VMEM((rows, 2 * pad), f32),
            pltpu.SemaphoreType.DMA((4,)),
            pltpu.SemaphoreType.DMA((rows // 2,)),
            pltpu.SemaphoreType.DMA((ring - 1, rows // 2)),
            pltpu.SemaphoreType.DMA((ring - 1, rows // 2)),
        ],
        compiler_params=pltpu.CompilerParams(collective_id=0, has_side_effects=True, vmem_limit_bytes=48 * 1024 * 1024),
        name="filter",
    )(*inputs)


def solution(mesh):
    return jax.shard_map(
        functools.partial(local, mesh.shape["lon"], mesh.shape["lat"]),
        mesh=mesh,
        in_specs=(P("lat", "lon", None), P("lat")),
        out_specs=P("lat", "lon", None),
        check_vma=False,
    )
```

```python
import functools

import jax
import jax.numpy as jnp
import numpy as np
from jax import lax
from jax.experimental import pallas as pl
from jax.experimental.pallas import tpu as pltpu
from jax.sharding import PartitionSpec as P

LANES = 128
SHAPES = 15
SLOT = 2 * SHAPES + 2
PER_TILE = LANES // SLOT
NEAR_RANK, FAR_RANK = 12, 4
MESH = pl.DeviceIdType.MESH


def filter_lines(cuts, length):
    wave = np.arange(length)
    folded = np.minimum(wave, length - wave)
    sine = np.sin(np.pi * np.maximum(folded, 1) / length)
    cuts = np.asarray(cuts)[:, None]
    gain = np.where(folded[None] <= cuts, 1.0, (np.sin(np.pi * cuts / length) / sine[None]) ** 2)
    return np.fft.ifft(gain, axis=1).real


def hankel(line, segment, distance):
    first = segment * distance - (segment - 1)
    wrapped = np.take(line, np.arange(first, first + 2 * segment - 1), mode="wrap")
    return np.lib.stride_tricks.sliding_window_view(wrapped, segment)


def envelope_shapes(length, segment, top):
    spot = np.arange(segment)
    family = [(a / (spot + a)) ** p for a in np.geomspace(0.3, 2 * segment, 40) for p in (1, 2, 3)]
    unit = 2.0 * spot / (segment - 1) - 1.0
    family += [np.polynomial.chebyshev.chebval(unit, [0] * j + [1]) for j in range(8)]
    left, size, _ = np.linalg.svd(np.array(family).T, full_matrices=False)
    left = left[:, size > 1e-6 * size[0]]
    cuts = np.unique(np.round(np.geomspace(1, top, 40)).astype(int))
    parts = []
    for cut, line in zip(cuts, filter_lines(cuts, length)):
        turn = 2.0 * np.pi * cut / length * spot[:, None]
        both = np.concatenate([left * np.cos(turn), left * np.sin(turn)], axis=1)
        u, s, vt = np.linalg.svd(both, full_matrices=False)
        keep = s > 1e-5 * s[0]
        inverse = (vt[keep].T / s[keep]) @ u[:, keep].T
        for distance in range(1, min(length // segment // 2, 4) + 1):
            u, s, _ = np.linalg.svd(inverse @ hankel(line, segment, distance), full_matrices=False)
            scaled = (u * s)[:, s > 1e-7]
            parts += [scaled[: left.shape[1]], scaled[left.shape[1] :]]
    u, _, _ = np.linalg.svd(np.concatenate(parts, axis=1), full_matrices=False)
    shapes = left @ u[:, :SHAPES]
    return np.pad(shapes, ((0, 0), (0, SHAPES - shapes.shape[1])))


@functools.lru_cache(maxsize=None)
def filter_tables(length, segment, top):
    shapes = envelope_shapes(length, segment, top)
    spot = np.arange(segment)
    cuts = np.arange(1, top + 1)
    lines = filter_lines(cuts, length)
    half = length // segment // 2
    ranks = [NEAR_RANK] + [FAR_RANK] * (half - 1)
    mixing = np.zeros((-(-(top + 1) // PER_TILE), sum(ranks), LANES))
    for cut, line in zip(cuts, lines):
        turn = 2.0 * np.pi * ((cut * spot) % length)[:, None] / length
        both = np.concatenate([shapes * np.cos(turn), shapes * np.sin(turn)], axis=1)
        u, s, vt = np.linalg.svd(both, full_matrices=False)
        keep = s > 3e-4 * s[0]
        u, back = u[:, keep], vt[keep].T / s[keep]
        at, start = (cut % PER_TILE) * SLOT, 0
        for distance, rank in enumerate(ranks, 1):
            inner = u.T @ (hankel(line, segment, distance) @ u)
            size, vectors = np.linalg.eigh((inner + inner.T) / 2.0)
            order = np.argsort(-np.abs(size), kind="stable")[:rank]
            count = len(order)
            weights = (back @ vectors[:, order]).T
            here = mixing[cut // PER_TILE, start : start + count, at : at + SLOT]
            here[:, :SHAPES] = weights[:, :SHAPES]
            here[:, SHAPES + 1 : 2 * SHAPES + 1] = weights[:, SHAPES:]
            here[:, SHAPES] = size[order]
            start += rank
    padded = -(-segment // LANES) * LANES
    tiles = padded // LANES
    halves = np.zeros((-(-(top + 1) // 8) * 8, tiles * LANES))
    halves[1 : top + 1] = lines[:, : tiles * LANES]
    halves = halves.reshape(-1, 8 * tiles, LANES)
    banks = np.zeros((2, SHAPES + 1, padded))
    banks[0, :SHAPES, :segment] = shapes.T
    banks[1, :SHAPES, :segment] = shapes[::-1].T
    near = np.concatenate([mixing[:, :NEAR_RANK], np.zeros((mixing.shape[0] % 2, NEAR_RANK, LANES))], axis=0)
    near = near.reshape(-1, 2 * NEAR_RANK, LANES)
    return [a.astype(np.float32) for a in (halves, near, mixing[:, NEAR_RANK:], banks)], ranks


def split(a):
    hi = a.astype(jnp.bfloat16)
    lo = (a - hi.astype(jnp.float32)).astype(jnp.bfloat16)
    return hi, lo


def polar_row(band, bands, rows, i):
    total = rows * bands
    return jnp.abs(2 * (band * rows + i) + 1 - total) * 5 > 2 * total


class Layout:
    def __init__(self, rows, segment, channels, ring, ranks):
        self.rows, self.segment, self.channels, self.ring = rows, segment, channels, ring
        self.padded = -(-segment // LANES) * LANES
        self.half = ring // 2
        self.tall = -(-segment // 16) * 16
        self.ranks = ranks
        self.count = sum(ranks)
        starts = np.concatenate([[0], np.cumsum(ranks)]).astype(int)
        self.far = self.count - NEAR_RANK

        def row(d, flip):
            return NEAR_RANK * flip if d == 1 else int(2 * NEAR_RANK + self.far * flip + starts[d - 1] - NEAR_RANK)

        self.unused = row(self.half, 1)
        plus = [(d, row(d, 1), row(d, 0), ranks[d - 1], d == 1) for d in range(1, self.half + 1)]
        minus = [(ring - d, row(d, 0), row(d, 1), ranks[d - 1], d == 1) for d in range(1, self.half)]
        self.peers, at = [], 0
        for step, send_row, come_row, rank, near in sorted(plus + minus, key=lambda peer: not peer[4]):
            self.peers.append((step, send_row, come_row, rank, at))
            at += rank * rows
        self.close = sum(peer[4] for peer in plus + minus)
        self.total = at


def three(a):
    hi = a.astype(jnp.bfloat16)
    rest = a - hi.astype(jnp.float32)
    mid = rest.astype(jnp.bfloat16)
    return hi, mid, (rest - mid.astype(jnp.float32)).astype(jnp.bfloat16)


def filter_kernel(lay, bands, top, cut_hbm, x_hbm, line_hbm, near_hbm, far_hbm, bank_hbm, y_ref, cut_ref, x_ref, line_ref, near_ref, far_ref, bank_ref, come_ref, m_ref, send, xs, left, turns, both, mt_ref, load_sem, x_sem, send_sem, recv_sem):
    seg, pad, ring, pairs = lay.segment, lay.padded, lay.ring, lay.rows // 2
    length = seg * ring
    band, me = lax.axis_index("lat"), lax.axis_index("lon")
    barrier = pltpu.get_barrier_semaphore()
    total = lay.rows * bands
    polar = [abs(2 * i + 1 - total) * 5 > 2 * total for i in range(total)]
    mixed_pairs = polar[0::2] != polar[1::2]

    def push(n, p):
        step, _, _, rank, at = lay.peers[n]
        rows = pl.ds(pl.multiple_of(at + 2 * rank * p, 8), 2 * rank)
        return pltpu.make_async_remote_copy(
            src_ref=send.at[rows],
            dst_ref=come_ref.at[rows],
            send_sem=send_sem.at[n, p],
            recv_sem=recv_sem.at[n, p],
            device_id={"lon": lax.rem(me + step, ring)},
            device_id_type=MESH,
        )

    def fetch(p):
        return pltpu.make_async_copy(x_hbm.at[pl.ds(2 * p, 2)], x_ref.at[pl.ds(2 * p, 2)], x_sem.at[p])

    loads = [
        pltpu.make_async_copy(a, b, load_sem.at[k])
        for k, (a, b) in enumerate(((cut_hbm, cut_ref), (bank_hbm, bank_ref), (near_hbm, near_ref), (line_hbm, line_ref), (far_hbm, far_ref)))
    ]
    for copy in loads[:3] + [fetch(0), loads[4]]:
        copy.start()
    for step in range(1, ring):
        pl.semaphore_signal(barrier, inc=1, device_id={"lon": lax.rem(me + step, ring)}, device_id_type=MESH)

    if pad != seg:
        for r in range(lay.rows):
            for k in range(3):
                xs[r, k * pad + seg : (k + 1) * pad] = jnp.zeros((pad - seg, lay.channels), jnp.bfloat16)
    loads[0].wait()
    for copy in [fetch(1), loads[3]] + [fetch(p) for p in range(2, pairs)]:
        copy.start()
    row = lax.broadcasted_iota(jnp.int32, (lay.rows, pad), 0)
    spot = lax.broadcasted_iota(jnp.int32, (lay.rows, pad), 1).astype(jnp.float32)
    cut = jnp.zeros((lay.rows, pad), jnp.float32)
    for i in range(lay.rows):
        cut = jnp.where(row == i, jnp.clip(cut_ref[i], 1, top).astype(jnp.float32), cut)
    for f, place in enumerate((spot, (seg - 1.0) - spot)):
        turn = cut * place
        turn = turn - jnp.floor(turn * (1.0 / length)) * length
        angle = turn * (2.0 * np.pi / length)
        turns[2 * f] = jnp.cos(angle)
        turns[2 * f + 1] = jnp.sin(angle)
    def halve(i):
        hi, lo = split(x_ref[i])
        xs[i, 0:seg] = hi
        xs[i, pad : pad + seg] = hi
        xs[i, 2 * pad : 2 * pad + seg] = lo

    def weights(i, far):
        cut = jnp.clip(cut_ref[i], 1, top)
        if far:
            mix = far_ref[cut // PER_TILE]
        else:
            mix = near_ref[cut // (2 * PER_TILE)]
            mix = jnp.where(lax.rem(cut // PER_TILE, 2) == 1, mix[NEAR_RANK:], mix[:NEAR_RANK])
        slot = lax.broadcasted_iota(jnp.int32, mix.shape, 1)
        mix = jnp.where(slot // SLOT == lax.rem(cut, PER_TILE), mix, 0.0)
        size = jnp.sum(jnp.where(lax.rem(slot, SLOT) == SHAPES, mix, 0.0), axis=1, keepdims=True)
        return functools.reduce(jnp.add, [mix[:, k * SLOT : (k + 1) * SLOT] for k in range(PER_TILE)]), size

    def project(i, parts):
        basis = []
        for f in range(2):
            basis.append(jnp.concatenate([bank_ref[f] * turns[2 * f + w, pl.ds(i, 1), :] for w in range(2)], axis=0))
        hi, mid, lo = three(jnp.concatenate(basis, axis=1))
        right = jnp.concatenate([hi, mid, lo, hi, mid, hi], axis=0)
        both_weights = [weights(i, far) for far in parts]
        hi, mid, lo = three(jnp.concatenate([w for w, _ in both_weights], axis=0))
        q = jnp.dot(jnp.concatenate([hi, hi, hi, mid, mid, lo], axis=1), right, preferred_element_type=jnp.float32)
        rows, at = [], 0
        for _, size in both_weights:
            part = q[at : at + size.shape[0]]
            rows += [part[:, :pad], part[:, pad:] * size]
            at += size.shape[0]
        hi, lo = split(jnp.concatenate(rows, axis=0))
        start, tops = (2 * NEAR_RANK if parts[0] else 0), 2 * at
        for k, part in enumerate((hi, lo, hi)):
            m_ref[i, start : start + tops, k * pad : (k + 1) * pad] = part
        two = jnp.dot(jnp.concatenate([hi, lo], axis=0), xs[i, :pad], preferred_element_type=jnp.float32)
        return two[:tops] + two[tops:] + jnp.dot(hi, xs[i, 2 * pad :], preferred_element_type=jnp.float32)

    def mirror():
        tiles = pad // LANES
        rows = []
        for i in range(lay.rows):
            cut = jnp.clip(cut_ref[i], 1, top)
            rows += [line_ref[cut // 8, pl.ds(lax.rem(cut, 8) * tiles + k, 1), :] for k in range(tiles)]
        ahead = jnp.concatenate(rows, axis=0)
        count = ahead.shape[0]
        lane = lax.broadcasted_iota(jnp.int32, (LANES, LANES), 0) + lax.broadcasted_iota(jnp.int32, (LANES, LANES), 1)
        turn = (lane == LANES).astype(jnp.bfloat16)
        back = jnp.dot(jnp.concatenate(three(ahead), axis=0), turn, preferred_element_type=jnp.float32)
        back = back[:count] + back[count : 2 * count] + back[2 * count :]
        ahead_next = jnp.concatenate([ahead[1:], ahead[:1]], axis=0)
        back = jnp.where(lax.broadcasted_iota(jnp.int32, back.shape, 1) == 0, ahead_next, back)
        for i in range(lay.rows):
            for k in range(tiles):
                at = i * tiles + k
                both[pl.ds(i, 1), (tiles - 1 - k) * LANES : (tiles - k) * LANES] = back[at : at + 1]
                both[pl.ds(i, 1), (tiles + k) * LANES : (tiles + k + 1) * LANES] = ahead[at : at + 1]

    def toeplitz(i, s):
        line = jnp.broadcast_to(both[pl.ds(i, 1), :], (LANES, 2 * pad))
        sheet = pltpu.roll(line, 2 * pad - LANES, 1, stride=1, stride_axis=0)[:, : 2 * pad - LANES]
        hi, lo = split(sheet)
        for q in range(pad // LANES):
            cols = slice(pad - LANES * (q + 1), 2 * pad - LANES * (q + 1))
            rows = min(LANES, lay.tall - q * LANES)
            block = slice(q * LANES, q * LANES + rows)
            left[s, block, 0:pad] = hi[:rows, cols]
            left[s, block, pad : 2 * pad] = lo[:rows, cols]
            left[s, block, 2 * pad : 3 * pad] = hi[:rows, cols]

    def post(p, parts):
        first, second = [project(2 * p + r, parts) for r in range(2)]
        which = range(0 if not parts[0] else lay.close, ring - 1 if parts[-1] else lay.close)
        shift = 2 * NEAR_RANK if parts[0] else 0
        for n in which:
            _, row, _, rank, at = lay.peers[n]
            row = row - shift
            two = jnp.concatenate([first[row : row + rank], second[row : row + rank]], axis=0)
            send[pl.ds(pl.multiple_of(at + 2 * rank * p, 8), 2 * rank), :] = two
        return which

    def finish(i, r, come):
        parts = [None] * (2 * lay.count)
        for (_, _, at_row, rank, _), both in zip(lay.peers, come):
            parts[at_row] = both[r * rank : (r + 1) * rank]
        parts[lay.unused] = jnp.zeros((lay.ranks[-1], lay.channels), jnp.float32)
        hi, lo = split(jnp.concatenate([v for v in parts if v is not None], axis=0))
        right = jnp.concatenate([hi, hi, lo], axis=0)
        far = jnp.dot(mt_ref[i], right, preferred_element_type=jnp.float32)[:seg]
        y = y_ref[i] + far
        y_ref[i] = jnp.where(polar_row(band, bands, lay.rows, i), y, x_ref[i]) if mixed_pairs else y

    loads[1].wait()
    loads[2].wait()
    fetch(0).wait()
    halve(0)
    halve(1)
    close = post(0, (0,))
    pl.semaphore_wait(barrier, ring - 1)
    for n in close:
        push(n, 0).start()
    loads[4].wait()
    for n in post(0, (1,)):
        push(n, 0).start()

    @pl.loop(1, pairs)
    def _(p):
        fetch(p).wait()
        halve(2 * p)
        halve(2 * p + 1)
        for n in post(p, (0, 1)):
            push(n, p).start()

    loads[3].wait()
    mirror()

    for i in range(lay.rows):
        toeplitz(i, i % 2)
        mt_ref[i] = jnp.concatenate([m_ref[i, :, k * pad : (k + 1) * pad] for k in range(3)], axis=0).T
        y_ref[i] = jnp.dot(left[i % 2], xs[i], preferred_element_type=jnp.float32)[:seg]

    @pl.loop(0, pairs)
    def _(p):
        for n in range(ring - 1):
            push(n, p).wait()
        any_on = jnp.logical_or(polar_row(band, bands, lay.rows, 2 * p), polar_row(band, bands, lay.rows, 2 * p + 1))

        @pl.when(any_on)
        def _():
            come = [come_ref[pl.ds(pl.multiple_of(at + 2 * rank * p, 8), 2 * rank), :] for _, _, _, rank, at in lay.peers]
            finish(2 * p, 0, come)
            finish(2 * p + 1, 1, come)

        @pl.when(jnp.logical_not(any_on))
        def _():
            y_ref[pl.ds(2 * p, 2)] = x_ref[pl.ds(2 * p, 2)]


def local(ring, bands, fields, cutoff):
    rows, segment, channels = fields.shape
    length, total = ring * segment, rows * bands
    row_ids = np.arange(total)
    polar = np.abs(2 * row_ids + 1 - total) * 5 > 2 * total
    poles = np.minimum(row_ids, total - 1 - row_ids)
    top = int(1 + (length // 2 - 1) * (2 * poles[polar].max() + 1) // total)
    tables, ranks = filter_tables(length, segment, top)
    lay = Layout(rows, segment, channels, ring, ranks)
    pad = lay.padded
    f32, bf16 = jnp.float32, jnp.bfloat16
    hbm = pl.BlockSpec(memory_space=pltpu.HBM)
    inputs = [pltpu.with_memory_space_constraint(a, pltpu.HBM) for a in (cutoff, fields, *map(jnp.asarray, tables))]
    return pl.pallas_call(
        functools.partial(filter_kernel, lay, bands, top),
        out_shape=jax.ShapeDtypeStruct(fields.shape, fields.dtype),
        in_specs=[hbm] * 6,
        out_specs=pl.BlockSpec(memory_space=pltpu.VMEM),
        scratch_shapes=[
            pltpu.SMEM((rows,), jnp.int32),
            pltpu.VMEM(fields.shape, f32),
            *[pltpu.VMEM(a.shape, f32) for a in tables],
            pltpu.VMEM((lay.total, channels), f32),
            pltpu.VMEM((rows, 2 * lay.count, 3 * pad), bf16),
            pltpu.VMEM((lay.total, channels), f32),
            pltpu.VMEM((rows, 3 * pad, channels), bf16),
            pltpu.VMEM((2, lay.tall, 3 * pad), bf16),
            pltpu.VMEM((4, rows, pad), f32),
            pltpu.VMEM((rows, 2 * pad), f32),
            pltpu.VMEM((rows, pad, 6 * lay.count), bf16),
            pltpu.SemaphoreType.DMA((5,)),
            pltpu.SemaphoreType.DMA((rows // 2,)),
            pltpu.SemaphoreType.DMA((ring - 1, rows // 2)),
            pltpu.SemaphoreType.DMA((ring - 1, rows // 2)),
        ],
        compiler_params=pltpu.CompilerParams(collective_id=0, has_side_effects=True, vmem_limit_bytes=48 * 1024 * 1024),
        name="filter",
    )(*inputs)


def solution(mesh):
    return jax.shard_map(
        functools.partial(local, mesh.shape["lon"], mesh.shape["lat"]),
        mesh=mesh,
        in_specs=(P("lat", "lon", None), P("lat")),
        out_specs=P("lat", "lon", None),
        check_vma=False,
    )
```

```python
import functools

import jax
import jax.numpy as jnp
import numpy as np
from jax import lax
from jax.experimental import pallas as pl
from jax.experimental.pallas import tpu as pltpu
from jax.sharding import PartitionSpec as P

LANES = 128
SHAPES = 15
SLOT = 2 * SHAPES + 2
PER_TILE = LANES // SLOT
NEAR_RANK, FAR_RANK = 12, 4
MESH = pl.DeviceIdType.MESH


def filter_lines(cuts, length):
    wave = np.arange(length)
    folded = np.minimum(wave, length - wave)
    sine = np.sin(np.pi * np.maximum(folded, 1) / length)
    cuts = np.asarray(cuts)[:, None]
    gain = np.where(folded[None] <= cuts, 1.0, (np.sin(np.pi * cuts / length) / sine[None]) ** 2)
    return np.fft.ifft(gain, axis=1).real


def hankel(line, segment, distance):
    first = segment * distance - (segment - 1)
    wrapped = np.take(line, np.arange(first, first + 2 * segment - 1), mode="wrap")
    return np.lib.stride_tricks.sliding_window_view(wrapped, segment)


def envelope_shapes(length, segment, top):
    spot = np.arange(segment)
    family = [(a / (spot + a)) ** p for a in np.geomspace(0.3, 2 * segment, 40) for p in (1, 2, 3)]
    unit = 2.0 * spot / (segment - 1) - 1.0
    family += [np.polynomial.chebyshev.chebval(unit, [0] * j + [1]) for j in range(8)]
    left, size, _ = np.linalg.svd(np.array(family).T, full_matrices=False)
    left = left[:, size > 1e-6 * size[0]]
    cuts = np.unique(np.round(np.geomspace(1, top, 40)).astype(int))
    parts = []
    for cut, line in zip(cuts, filter_lines(cuts, length)):
        turn = 2.0 * np.pi * cut / length * spot[:, None]
        both = np.concatenate([left * np.cos(turn), left * np.sin(turn)], axis=1)
        u, s, vt = np.linalg.svd(both, full_matrices=False)
        keep = s > 1e-5 * s[0]
        inverse = (vt[keep].T / s[keep]) @ u[:, keep].T
        for distance in range(1, min(length // segment // 2, 4) + 1):
            u, s, _ = np.linalg.svd(inverse @ hankel(line, segment, distance), full_matrices=False)
            scaled = (u * s)[:, s > 1e-7]
            parts += [scaled[: left.shape[1]], scaled[left.shape[1] :]]
    u, _, _ = np.linalg.svd(np.concatenate(parts, axis=1), full_matrices=False)
    shapes = left @ u[:, :SHAPES]
    return np.pad(shapes, ((0, 0), (0, SHAPES - shapes.shape[1])))


@functools.lru_cache(maxsize=None)
def filter_tables(length, segment, top):
    shapes = envelope_shapes(length, segment, top)
    spot = np.arange(segment)
    cuts = np.arange(1, top + 1)
    lines = filter_lines(cuts, length)
    half = length // segment // 2
    ranks = [NEAR_RANK] + [FAR_RANK] * (half - 1)
    mixing = np.zeros((-(-(top + 1) // PER_TILE), sum(ranks), LANES))
    for cut, line in zip(cuts, lines):
        turn = 2.0 * np.pi * ((cut * spot) % length)[:, None] / length
        both = np.concatenate([shapes * np.cos(turn), shapes * np.sin(turn)], axis=1)
        u, s, vt = np.linalg.svd(both, full_matrices=False)
        keep = s > 3e-4 * s[0]
        u, back = u[:, keep], vt[keep].T / s[keep]
        at, start = (cut % PER_TILE) * SLOT, 0
        for distance, rank in enumerate(ranks, 1):
            inner = u.T @ (hankel(line, segment, distance) @ u)
            size, vectors = np.linalg.eigh((inner + inner.T) / 2.0)
            order = np.argsort(-np.abs(size), kind="stable")[:rank]
            count = len(order)
            weights = (back @ vectors[:, order]).T
            here = mixing[cut // PER_TILE, start : start + count, at : at + SLOT]
            here[:, :SHAPES] = weights[:, :SHAPES]
            here[:, SHAPES + 1 : 2 * SHAPES + 1] = weights[:, SHAPES:]
            here[:, SHAPES] = size[order]
            start += rank
    padded = -(-segment // LANES) * LANES
    tiles = padded // LANES
    halves = np.zeros((-(-(top + 1) // 8) * 8, tiles * LANES))
    halves[1 : top + 1] = lines[:, : tiles * LANES]
    halves = halves.reshape(-1, 8 * tiles, LANES)
    banks = np.zeros((2, SHAPES + 1, padded))
    banks[0, :SHAPES, :segment] = shapes.T
    banks[1, :SHAPES, :segment] = shapes[::-1].T
    return halves.astype(np.float32), mixing.astype(np.float32), banks.astype(np.float32), ranks


def split(a):
    hi = a.astype(jnp.bfloat16)
    lo = (a - hi.astype(jnp.float32)).astype(jnp.bfloat16)
    return hi, lo


def polar_row(band, bands, rows, i):
    total = rows * bands
    return jnp.abs(2 * (band * rows + i) + 1 - total) * 5 > 2 * total


class Layout:
    def __init__(self, rows, segment, channels, ring, ranks):
        self.rows, self.segment, self.channels, self.ring = rows, segment, channels, ring
        self.padded = -(-segment // LANES) * LANES
        self.half = ring // 2
        self.tall = -(-segment // 16) * 16
        self.ranks = ranks
        self.count = sum(ranks)
        starts = np.concatenate([[0], np.cumsum(ranks)]).astype(int)
        plus = [(d, self.count + starts[d - 1], starts[d - 1], ranks[d - 1]) for d in range(1, self.half + 1)]
        minus = [(ring - d, starts[d - 1], self.count + starts[d - 1], ranks[d - 1]) for d in range(1, self.half)]
        self.peers, at = [], 0
        for step, send_row, come_row, rank in plus + minus:
            self.peers.append((step, int(send_row), int(come_row), rank, at))
            at += rank * rows
        self.total = at


def three(a):
    hi = a.astype(jnp.bfloat16)
    rest = a - hi.astype(jnp.float32)
    mid = rest.astype(jnp.bfloat16)
    return hi, mid, (rest - mid.astype(jnp.float32)).astype(jnp.bfloat16)


def filter_kernel(lay, bands, top, cut_hbm, x_hbm, line_hbm, mix_hbm, bank_hbm, y_ref, cut_ref, x_ref, line_ref, mix_ref, bank_ref, come_ref, m_ref, send, xs, left, turns, both, mt_ref, load_sem, x_sem, send_sem, recv_sem):
    seg, pad, ring, pairs = lay.segment, lay.padded, lay.ring, lay.rows // 2
    length = seg * ring
    band, me = lax.axis_index("lat"), lax.axis_index("lon")
    barrier = pltpu.get_barrier_semaphore()
    total = lay.rows * bands
    polar = [abs(2 * i + 1 - total) * 5 > 2 * total for i in range(total)]
    mixed_pairs = polar[0::2] != polar[1::2]

    def push(n, p):
        step, _, _, rank, at = lay.peers[n]
        rows = pl.ds(pl.multiple_of(at + 2 * rank * p, 8), 2 * rank)
        return pltpu.make_async_remote_copy(
            src_ref=send.at[rows],
            dst_ref=come_ref.at[rows],
            send_sem=send_sem.at[n, p],
            recv_sem=recv_sem.at[n, p],
            device_id={"lon": lax.rem(me + step, ring)},
            device_id_type=MESH,
        )

    def fetch(p):
        return pltpu.make_async_copy(x_hbm.at[pl.ds(2 * p, 2)], x_ref.at[pl.ds(2 * p, 2)], x_sem.at[p])

    loads = [
        pltpu.make_async_copy(a, b, load_sem.at[k])
        for k, (a, b) in enumerate(((cut_hbm, cut_ref), (bank_hbm, bank_ref), (mix_hbm, mix_ref), (line_hbm, line_ref)))
    ]
    for copy in loads[:3]:
        copy.start()
    fetch(0).start()
    for step in range(1, ring):
        pl.semaphore_signal(barrier, inc=1, device_id={"lon": lax.rem(me + step, ring)}, device_id_type=MESH)

    if pad != seg:
        for r in range(lay.rows):
            for k in range(3):
                xs[r, k * pad + seg : (k + 1) * pad] = jnp.zeros((pad - seg, lay.channels), jnp.bfloat16)
    loads[0].wait()
    for copy in [fetch(1), loads[3]] + [fetch(p) for p in range(2, pairs)]:
        copy.start()
    row = lax.broadcasted_iota(jnp.int32, (lay.rows, pad), 0)
    spot = lax.broadcasted_iota(jnp.int32, (lay.rows, pad), 1).astype(jnp.float32)
    cut = jnp.zeros((lay.rows, pad), jnp.float32)
    for i in range(lay.rows):
        cut = jnp.where(row == i, jnp.clip(cut_ref[i], 1, top).astype(jnp.float32), cut)
    for f, place in enumerate((spot, (seg - 1.0) - spot)):
        turn = cut * place
        turn = turn - jnp.floor(turn * (1.0 / length)) * length
        angle = turn * (2.0 * np.pi / length)
        turns[2 * f] = jnp.cos(angle)
        turns[2 * f + 1] = jnp.sin(angle)
    slot = lax.broadcasted_iota(jnp.int32, (lay.count, LANES), 1)
    loads[1].wait()
    loads[2].wait()

    def mixed(i):
        x = x_ref[i]
        hi, lo = split(x)
        xs[i, 0:seg] = hi
        xs[i, pad : pad + seg] = hi
        xs[i, 2 * pad : 2 * pad + seg] = lo
        basis = []
        for f in range(2):
            basis.append(jnp.concatenate([bank_ref[f] * turns[2 * f + w, pl.ds(i, 1), :] for w in range(2)], axis=0))
        hi, mid, lo = three(jnp.concatenate(basis, axis=1))
        right = jnp.concatenate([hi, mid, lo, hi, mid, hi], axis=0)
        cut = jnp.clip(cut_ref[i], 1, top)
        mix = jnp.where(slot // SLOT == lax.rem(cut, PER_TILE), mix_ref[cut // PER_TILE], 0.0)
        size = jnp.sum(jnp.where(lax.rem(slot, SLOT) == SHAPES, mix, 0.0), axis=1, keepdims=True)
        mix = functools.reduce(jnp.add, [mix[:, k * SLOT : (k + 1) * SLOT] for k in range(PER_TILE)])
        hi, mid, lo = three(mix)
        q = jnp.dot(jnp.concatenate([hi, hi, hi, mid, mid, lo], axis=1), right, preferred_element_type=jnp.float32)
        hi, lo = split(jnp.concatenate([q[:, :pad], q[:, pad:] * size], axis=0))
        m = jnp.concatenate([hi, lo, hi], axis=1)
        m_ref[i] = m
        return m

    def project(i):
        m = mixed(i)
        tops = 2 * lay.count
        two = jnp.dot(jnp.concatenate([m[:, :pad], m[:, pad : 2 * pad]], axis=0), xs[i, :pad], preferred_element_type=jnp.float32)
        return two[:tops] + two[tops:] + jnp.dot(m[:, :pad], xs[i, 2 * pad :], preferred_element_type=jnp.float32)

    def mirror():
        tiles = pad // LANES
        rows = []
        for i in range(lay.rows):
            cut = jnp.clip(cut_ref[i], 1, top)
            rows += [line_ref[cut // 8, pl.ds(lax.rem(cut, 8) * tiles + k, 1), :] for k in range(tiles)]
        ahead = jnp.concatenate(rows, axis=0)
        count = ahead.shape[0]
        lane = lax.broadcasted_iota(jnp.int32, (LANES, LANES), 0) + lax.broadcasted_iota(jnp.int32, (LANES, LANES), 1)
        turn = (lane == LANES).astype(jnp.bfloat16)
        back = jnp.dot(jnp.concatenate(three(ahead), axis=0), turn, preferred_element_type=jnp.float32)
        back = back[:count] + back[count : 2 * count] + back[2 * count :]
        ahead_next = jnp.concatenate([ahead[1:], ahead[:1]], axis=0)
        back = jnp.where(lax.broadcasted_iota(jnp.int32, back.shape, 1) == 0, ahead_next, back)
        for i in range(lay.rows):
            for k in range(tiles):
                at = i * tiles + k
                both[pl.ds(i, 1), (tiles - 1 - k) * LANES : (tiles - k) * LANES] = back[at : at + 1]
                both[pl.ds(i, 1), (tiles + k) * LANES : (tiles + k + 1) * LANES] = ahead[at : at + 1]

    def toeplitz(i, s):
        line = jnp.broadcast_to(both[pl.ds(i, 1), :], (LANES, 2 * pad))
        sheet = pltpu.roll(line, 2 * pad - LANES, 1, stride=1, stride_axis=0)[:, : 2 * pad - LANES]
        hi, lo = split(sheet)
        for q in range(pad // LANES):
            cols = slice(pad - LANES * (q + 1), 2 * pad - LANES * (q + 1))
            rows = min(LANES, lay.tall - q * LANES)
            block = slice(q * LANES, q * LANES + rows)
            left[s, block, 0:pad] = hi[:rows, cols]
            left[s, block, pad : 2 * pad] = lo[:rows, cols]
            left[s, block, 2 * pad : 3 * pad] = hi[:rows, cols]

    def post(p, first, second):
        for _, at_row, _, rank, at in lay.peers:
            two = jnp.concatenate([first[at_row : at_row + rank], second[at_row : at_row + rank]], axis=0)
            send[pl.ds(pl.multiple_of(at + 2 * rank * p, 8), 2 * rank), :] = two

    def finish(i, r, come):
        parts = [None] * (2 * lay.count)
        for (_, _, at_row, rank, _), both in zip(lay.peers, come):
            parts[at_row] = both[r * rank : (r + 1) * rank]
        unused = lay.count + sum(lay.ranks[:-1])
        parts[unused] = jnp.zeros((lay.ranks[-1], lay.channels), jnp.float32)
        hi, lo = split(jnp.concatenate([v for v in parts if v is not None], axis=0))
        right = jnp.concatenate([hi, hi, lo], axis=0)
        far = jnp.dot(mt_ref[i], right, preferred_element_type=jnp.float32)[:seg]
        y = y_ref[i] + far
        y_ref[i] = jnp.where(polar_row(band, bands, lay.rows, i), y, x_ref[i]) if mixed_pairs else y

    @pl.loop(0, pairs)
    def _(p):
        fetch(p).wait()
        post(p, *[project(2 * p + r) for r in range(2)])

        @pl.when(p == 0)
        def _():
            pl.semaphore_wait(barrier, ring - 1)

        for n in range(ring - 1):
            push(n, p).start()

    loads[3].wait()
    mirror()

    for i in range(lay.rows):
        toeplitz(i, i % 2)
        mt_ref[i] = jnp.concatenate([m_ref[i, :, k * pad : (k + 1) * pad] for k in range(3)], axis=0).T
        y_ref[i] = jnp.dot(left[i % 2], xs[i], preferred_element_type=jnp.float32)[:seg]

    @pl.loop(0, pairs)
    def _(p):
        for n in range(ring - 1):
            push(n, p).wait()
        any_on = jnp.logical_or(polar_row(band, bands, lay.rows, 2 * p), polar_row(band, bands, lay.rows, 2 * p + 1))

        @pl.when(any_on)
        def _():
            come = [come_ref[pl.ds(pl.multiple_of(at + 2 * rank * p, 8), 2 * rank), :] for _, _, _, rank, at in lay.peers]
            finish(2 * p, 0, come)
            finish(2 * p + 1, 1, come)

        @pl.when(jnp.logical_not(any_on))
        def _():
            y_ref[pl.ds(2 * p, 2)] = x_ref[pl.ds(2 * p, 2)]


def local(ring, bands, fields, cutoff):
    rows, segment, channels = fields.shape
    length, total = ring * segment, rows * bands
    row_ids = np.arange(total)
    polar = np.abs(2 * row_ids + 1 - total) * 5 > 2 * total
    poles = np.minimum(row_ids, total - 1 - row_ids)
    top = int(1 + (length // 2 - 1) * (2 * poles[polar].max() + 1) // total)
    lines, mixing, bank, ranks = filter_tables(length, segment, top)
    lay = Layout(rows, segment, channels, ring, ranks)
    pad = lay.padded
    f32, bf16 = jnp.float32, jnp.bfloat16
    hbm = pl.BlockSpec(memory_space=pltpu.HBM)
    inputs = [pltpu.with_memory_space_constraint(a, pltpu.HBM) for a in (cutoff, fields, *map(jnp.asarray, (lines, mixing, bank)))]
    return pl.pallas_call(
        functools.partial(filter_kernel, lay, bands, top),
        out_shape=jax.ShapeDtypeStruct(fields.shape, fields.dtype),
        in_specs=[hbm] * 5,
        out_specs=pl.BlockSpec(memory_space=pltpu.VMEM),
        scratch_shapes=[
            pltpu.SMEM((rows,), jnp.int32),
            pltpu.VMEM(fields.shape, f32),
            pltpu.VMEM(lines.shape, f32),
            pltpu.VMEM(mixing.shape, f32),
            pltpu.VMEM(bank.shape, f32),
            pltpu.VMEM((lay.total, channels), f32),
            pltpu.VMEM((rows, 2 * lay.count, 3 * pad), bf16),
            pltpu.VMEM((lay.total, channels), f32),
            pltpu.VMEM((rows, 3 * pad, channels), bf16),
            pltpu.VMEM((2, lay.tall, 3 * pad), bf16),
            pltpu.VMEM((4, rows, pad), f32),
            pltpu.VMEM((rows, 2 * pad), f32),
            pltpu.VMEM((rows, pad, 6 * lay.count), bf16),
            pltpu.SemaphoreType.DMA((4,)),
            pltpu.SemaphoreType.DMA((rows // 2,)),
            pltpu.SemaphoreType.DMA((ring - 1, rows // 2)),
            pltpu.SemaphoreType.DMA((ring - 1, rows // 2)),
        ],
        compiler_params=pltpu.CompilerParams(collective_id=0, has_side_effects=True, vmem_limit_bytes=48 * 1024 * 1024),
        name="filter",
    )(*inputs)


def solution(mesh):
    return jax.shard_map(
        functools.partial(local, mesh.shape["lon"], mesh.shape["lat"]),
        mesh=mesh,
        in_specs=(P("lat", "lon", None), P("lat")),
        out_specs=P("lat", "lon", None),
        check_vma=False,
    )
```

```python
import functools

import jax
import jax.numpy as jnp
import numpy as np
from jax import lax
from jax.experimental import pallas as pl
from jax.experimental.pallas import tpu as pltpu
from jax.sharding import PartitionSpec as P

LANES = 128
SHAPES = 15
SLOT = 2 * SHAPES + 2
PER_TILE = LANES // SLOT
NEAR_RANK, FAR_RANK = 12, 4
MESH = pl.DeviceIdType.MESH


def filter_lines(cuts, length):
    wave = np.arange(length)
    folded = np.minimum(wave, length - wave)
    sine = np.sin(np.pi * np.maximum(folded, 1) / length)
    cuts = np.asarray(cuts)[:, None]
    gain = np.where(folded[None] <= cuts, 1.0, (np.sin(np.pi * cuts / length) / sine[None]) ** 2)
    return np.fft.ifft(gain, axis=1).real


def hankel(line, segment, distance):
    first = segment * distance - (segment - 1)
    wrapped = np.take(line, np.arange(first, first + 2 * segment - 1), mode="wrap")
    return np.lib.stride_tricks.sliding_window_view(wrapped, segment)


def envelope_shapes(length, segment, top):
    spot = np.arange(segment)
    family = [(a / (spot + a)) ** p for a in np.geomspace(0.3, 2 * segment, 40) for p in (1, 2, 3)]
    unit = 2.0 * spot / (segment - 1) - 1.0
    family += [np.polynomial.chebyshev.chebval(unit, [0] * j + [1]) for j in range(8)]
    left, size, _ = np.linalg.svd(np.array(family).T, full_matrices=False)
    left = left[:, size > 1e-6 * size[0]]
    cuts = np.unique(np.round(np.geomspace(1, top, 40)).astype(int))
    parts = []
    for cut, line in zip(cuts, filter_lines(cuts, length)):
        turn = 2.0 * np.pi * cut / length * spot[:, None]
        both = np.concatenate([left * np.cos(turn), left * np.sin(turn)], axis=1)
        u, s, vt = np.linalg.svd(both, full_matrices=False)
        keep = s > 1e-5 * s[0]
        inverse = (vt[keep].T / s[keep]) @ u[:, keep].T
        for distance in range(1, min(length // segment // 2, 4) + 1):
            u, s, _ = np.linalg.svd(inverse @ hankel(line, segment, distance), full_matrices=False)
            scaled = (u * s)[:, s > 1e-7]
            parts += [scaled[: left.shape[1]], scaled[left.shape[1] :]]
    u, _, _ = np.linalg.svd(np.concatenate(parts, axis=1), full_matrices=False)
    shapes = left @ u[:, :SHAPES]
    return np.pad(shapes, ((0, 0), (0, SHAPES - shapes.shape[1])))


@functools.lru_cache(maxsize=None)
def filter_tables(length, segment, top):
    shapes = envelope_shapes(length, segment, top)
    spot = np.arange(segment)
    cuts = np.arange(1, top + 1)
    lines = filter_lines(cuts, length)
    half = length // segment // 2
    ranks = [NEAR_RANK] + [FAR_RANK] * (half - 1)
    mixing = np.zeros((-(-(top + 1) // PER_TILE), sum(ranks), LANES))
    for cut, line in zip(cuts, lines):
        turn = 2.0 * np.pi * ((cut * spot) % length)[:, None] / length
        both = np.concatenate([shapes * np.cos(turn), shapes * np.sin(turn)], axis=1)
        u, s, vt = np.linalg.svd(both, full_matrices=False)
        keep = s > 3e-4 * s[0]
        u, back = u[:, keep], vt[keep].T / s[keep]
        at, start = (cut % PER_TILE) * SLOT, 0
        for distance, rank in enumerate(ranks, 1):
            inner = u.T @ (hankel(line, segment, distance) @ u)
            size, vectors = np.linalg.eigh((inner + inner.T) / 2.0)
            order = np.argsort(-np.abs(size), kind="stable")[:rank]
            count = len(order)
            weights = (back @ vectors[:, order]).T
            here = mixing[cut // PER_TILE, start : start + count, at : at + SLOT]
            here[:, :SHAPES] = weights[:, :SHAPES]
            here[:, SHAPES + 1 : 2 * SHAPES + 1] = weights[:, SHAPES:]
            here[:, SHAPES] = size[order]
            start += rank
    padded = -(-segment // LANES) * LANES
    tiles = padded // LANES
    halves = np.zeros((-(-(top + 1) // 8) * 8, tiles * LANES))
    halves[1 : top + 1] = lines[:, : tiles * LANES]
    halves = halves.reshape(-1, 8 * tiles, LANES)
    banks = np.zeros((2, SHAPES + 1, padded))
    banks[0, :SHAPES, :segment] = shapes.T
    banks[1, :SHAPES, :segment] = shapes[::-1].T
    return halves.astype(np.float32), mixing.astype(np.float32), banks.astype(np.float32), ranks


def split(a):
    hi = a.astype(jnp.bfloat16)
    lo = (a - hi.astype(jnp.float32)).astype(jnp.bfloat16)
    return hi, lo


def polar_row(band, bands, rows, i):
    total = rows * bands
    return jnp.abs(2 * (band * rows + i) + 1 - total) * 5 > 2 * total


class Layout:
    def __init__(self, rows, segment, channels, ring, ranks):
        self.rows, self.segment, self.channels, self.ring = rows, segment, channels, ring
        self.padded = -(-segment // LANES) * LANES
        self.half = ring // 2
        self.tall = -(-segment // 16) * 16
        self.ranks = ranks
        self.count = sum(ranks)
        starts = np.concatenate([[0], np.cumsum(ranks)]).astype(int)
        plus = [(d, self.count + starts[d - 1], starts[d - 1], ranks[d - 1]) for d in range(1, self.half + 1)]
        minus = [(ring - d, starts[d - 1], self.count + starts[d - 1], ranks[d - 1]) for d in range(1, self.half)]
        self.peers, at = [], 0
        for step, send_row, come_row, rank in plus + minus:
            self.peers.append((step, int(send_row), int(come_row), rank, at))
            at += rank * rows
        self.total = at


def three(a):
    hi = a.astype(jnp.bfloat16)
    rest = a - hi.astype(jnp.float32)
    mid = rest.astype(jnp.bfloat16)
    return hi, mid, (rest - mid.astype(jnp.float32)).astype(jnp.bfloat16)


def filter_kernel(lay, bands, top, cut_hbm, x_hbm, line_hbm, mix_hbm, bank_hbm, y_ref, cut_ref, x_ref, line_ref, mix_ref, bank_ref, come_ref, m_ref, send, xs, left, turns, both, mt_ref, load_sem, mix_sem, x_sem, send_sem, recv_sem):
    seg, pad, ring, pairs = lay.segment, lay.padded, lay.ring, lay.rows // 2
    length = seg * ring
    band, me = lax.axis_index("lat"), lax.axis_index("lon")
    barrier = pltpu.get_barrier_semaphore()
    total = lay.rows * bands
    polar = [abs(2 * i + 1 - total) * 5 > 2 * total for i in range(total)]
    mixed_pairs = polar[0::2] != polar[1::2]

    def push(n, p):
        step, _, _, rank, at = lay.peers[n]
        rows = pl.ds(pl.multiple_of(at + 2 * rank * p, 8), 2 * rank)
        return pltpu.make_async_remote_copy(
            src_ref=send.at[rows],
            dst_ref=come_ref.at[rows],
            send_sem=send_sem.at[n, p],
            recv_sem=recv_sem.at[n, p],
            device_id={"lon": lax.rem(me + step, ring)},
            device_id_type=MESH,
        )

    def fetch(p):
        return pltpu.make_async_copy(x_hbm.at[pl.ds(2 * p, 2)], x_ref.at[pl.ds(2 * p, 2)], x_sem.at[p])

    loads = [
        pltpu.make_async_copy(a, b, load_sem.at[k])
        for k, (a, b) in enumerate(((cut_hbm, cut_ref), (bank_hbm, bank_ref), (line_hbm, line_ref)))
    ]
    groups = mix_hbm.shape[0]
    cuts_at = [groups * k // 4 for k in range(5)]
    mixes = [
        pltpu.make_async_copy(mix_hbm.at[pl.ds(a, b - a)], mix_ref.at[pl.ds(a, b - a)], mix_sem.at[k])
        for k, (a, b) in enumerate(zip(cuts_at, cuts_at[1:]))
    ]
    for copy in loads[:2] + mixes + [fetch(0)]:
        copy.start()
    for step in range(1, ring):
        pl.semaphore_signal(barrier, inc=1, device_id={"lon": lax.rem(me + step, ring)}, device_id_type=MESH)

    if pad != seg:
        for r in range(lay.rows):
            for k in range(3):
                xs[r, k * pad + seg : (k + 1) * pad] = jnp.zeros((pad - seg, lay.channels), jnp.bfloat16)
    loads[0].wait()
    for copy in [fetch(p) for p in range(1, pairs)] + [loads[2]]:
        copy.start()
    row = lax.broadcasted_iota(jnp.int32, (lay.rows, pad), 0)
    spot = lax.broadcasted_iota(jnp.int32, (lay.rows, pad), 1).astype(jnp.float32)
    cut = jnp.zeros((lay.rows, pad), jnp.float32)
    for i in range(lay.rows):
        cut = jnp.where(row == i, jnp.clip(cut_ref[i], 1, top).astype(jnp.float32), cut)
    for f, place in enumerate((spot, (seg - 1.0) - spot)):
        turn = cut * place
        turn = turn - jnp.floor(turn * (1.0 / length)) * length
        angle = turn * (2.0 * np.pi / length)
        turns[2 * f] = jnp.cos(angle)
        turns[2 * f + 1] = jnp.sin(angle)
    slot = lax.broadcasted_iota(jnp.int32, (lay.count, LANES), 1)
    loads[1].wait()
    for copy in mixes:
        copy.wait()

    def mixed(i):
        x = x_ref[i]
        hi, lo = split(x)
        xs[i, 0:seg] = hi
        xs[i, pad : pad + seg] = hi
        xs[i, 2 * pad : 2 * pad + seg] = lo
        basis = []
        for f in range(2):
            basis.append(jnp.concatenate([bank_ref[f] * turns[2 * f + w, pl.ds(i, 1), :] for w in range(2)], axis=0))
        hi, mid, lo = three(jnp.concatenate(basis, axis=1))
        right = jnp.concatenate([hi, mid, lo, hi, mid, hi], axis=0)
        cut = jnp.clip(cut_ref[i], 1, top)
        mix = jnp.where(slot // SLOT == lax.rem(cut, PER_TILE), mix_ref[cut // PER_TILE], 0.0)
        size = jnp.sum(jnp.where(lax.rem(slot, SLOT) == SHAPES, mix, 0.0), axis=1, keepdims=True)
        mix = functools.reduce(jnp.add, [mix[:, k * SLOT : (k + 1) * SLOT] for k in range(PER_TILE)])
        hi, mid, lo = three(mix)
        q = jnp.dot(jnp.concatenate([hi, hi, hi, mid, mid, lo], axis=1), right, preferred_element_type=jnp.float32)
        hi, lo = split(jnp.concatenate([q[:, :pad], q[:, pad:] * size], axis=0))
        m = jnp.concatenate([hi, lo, hi], axis=1)
        m_ref[i] = m
        return m

    def project(i):
        m = mixed(i)
        tops = 2 * lay.count
        two = jnp.dot(jnp.concatenate([m[:, :pad], m[:, pad : 2 * pad]], axis=0), xs[i, :pad], preferred_element_type=jnp.float32)
        return two[:tops] + two[tops:] + jnp.dot(m[:, :pad], xs[i, 2 * pad :], preferred_element_type=jnp.float32)

    def mirror():
        tiles = pad // LANES
        rows = []
        for i in range(lay.rows):
            cut = jnp.clip(cut_ref[i], 1, top)
            rows += [line_ref[cut // 8, pl.ds(lax.rem(cut, 8) * tiles + k, 1), :] for k in range(tiles)]
        ahead = jnp.concatenate(rows, axis=0)
        count = ahead.shape[0]
        lane = lax.broadcasted_iota(jnp.int32, (LANES, LANES), 0) + lax.broadcasted_iota(jnp.int32, (LANES, LANES), 1)
        turn = (lane == LANES).astype(jnp.bfloat16)
        back = jnp.dot(jnp.concatenate(three(ahead), axis=0), turn, preferred_element_type=jnp.float32)
        back = back[:count] + back[count : 2 * count] + back[2 * count :]
        ahead_next = jnp.concatenate([ahead[1:], ahead[:1]], axis=0)
        back = jnp.where(lax.broadcasted_iota(jnp.int32, back.shape, 1) == 0, ahead_next, back)
        for i in range(lay.rows):
            for k in range(tiles):
                at = i * tiles + k
                both[pl.ds(i, 1), (tiles - 1 - k) * LANES : (tiles - k) * LANES] = back[at : at + 1]
                both[pl.ds(i, 1), (tiles + k) * LANES : (tiles + k + 1) * LANES] = ahead[at : at + 1]

    def toeplitz(i, s):
        line = jnp.broadcast_to(both[pl.ds(i, 1), :], (LANES, 2 * pad))
        sheet = pltpu.roll(line, 2 * pad - LANES, 1, stride=1, stride_axis=0)[:, : 2 * pad - LANES]
        hi, lo = split(sheet)
        for q in range(pad // LANES):
            cols = slice(pad - LANES * (q + 1), 2 * pad - LANES * (q + 1))
            rows = min(LANES, lay.tall - q * LANES)
            block = slice(q * LANES, q * LANES + rows)
            left[s, block, 0:pad] = hi[:rows, cols]
            left[s, block, pad : 2 * pad] = lo[:rows, cols]
            left[s, block, 2 * pad : 3 * pad] = hi[:rows, cols]

    def post(p, first, second):
        for _, at_row, _, rank, at in lay.peers:
            two = jnp.concatenate([first[at_row : at_row + rank], second[at_row : at_row + rank]], axis=0)
            send[pl.ds(pl.multiple_of(at + 2 * rank * p, 8), 2 * rank), :] = two

    def finish(i, r, come):
        parts = [None] * (2 * lay.count)
        for (_, _, at_row, rank, _), both in zip(lay.peers, come):
            parts[at_row] = both[r * rank : (r + 1) * rank]
        unused = lay.count + sum(lay.ranks[:-1])
        parts[unused] = jnp.zeros((lay.ranks[-1], lay.channels), jnp.float32)
        hi, lo = split(jnp.concatenate([v for v in parts if v is not None], axis=0))
        right = jnp.concatenate([hi, hi, lo], axis=0)
        far = jnp.dot(mt_ref[i], right, preferred_element_type=jnp.float32)[:seg]
        y = y_ref[i] + far
        y_ref[i] = jnp.where(polar_row(band, bands, lay.rows, i), y, x_ref[i]) if mixed_pairs else y

    @pl.loop(0, pairs)
    def _(p):
        fetch(p).wait()
        post(p, *[project(2 * p + r) for r in range(2)])

        @pl.when(p == 0)
        def _():
            pl.semaphore_wait(barrier, ring - 1)

        for n in range(ring - 1):
            push(n, p).start()

    loads[2].wait()
    mirror()

    for i in range(lay.rows):
        toeplitz(i, i % 2)
        mt_ref[i] = jnp.concatenate([m_ref[i, :, k * pad : (k + 1) * pad] for k in range(3)], axis=0).T
        y_ref[i] = jnp.dot(left[i % 2], xs[i], preferred_element_type=jnp.float32)[:seg]

    @pl.loop(0, pairs)
    def _(p):
        for n in range(ring - 1):
            push(n, p).wait()
        any_on = jnp.logical_or(polar_row(band, bands, lay.rows, 2 * p), polar_row(band, bands, lay.rows, 2 * p + 1))

        @pl.when(any_on)
        def _():
            come = [come_ref[pl.ds(pl.multiple_of(at + 2 * rank * p, 8), 2 * rank), :] for _, _, _, rank, at in lay.peers]
            finish(2 * p, 0, come)
            finish(2 * p + 1, 1, come)

        @pl.when(jnp.logical_not(any_on))
        def _():
            y_ref[pl.ds(2 * p, 2)] = x_ref[pl.ds(2 * p, 2)]


def local(ring, bands, fields, cutoff):
    rows, segment, channels = fields.shape
    length, total = ring * segment, rows * bands
    row_ids = np.arange(total)
    polar = np.abs(2 * row_ids + 1 - total) * 5 > 2 * total
    poles = np.minimum(row_ids, total - 1 - row_ids)
    top = int(1 + (length // 2 - 1) * (2 * poles[polar].max() + 1) // total)
    lines, mixing, bank, ranks = filter_tables(length, segment, top)
    lay = Layout(rows, segment, channels, ring, ranks)
    pad = lay.padded
    f32, bf16 = jnp.float32, jnp.bfloat16
    hbm = pl.BlockSpec(memory_space=pltpu.HBM)
    inputs = [pltpu.with_memory_space_constraint(a, pltpu.HBM) for a in (cutoff, fields, *map(jnp.asarray, (lines, mixing, bank)))]
    return pl.pallas_call(
        functools.partial(filter_kernel, lay, bands, top),
        out_shape=jax.ShapeDtypeStruct(fields.shape, fields.dtype),
        in_specs=[hbm] * 5,
        out_specs=pl.BlockSpec(memory_space=pltpu.VMEM),
        scratch_shapes=[
            pltpu.SMEM((rows,), jnp.int32),
            pltpu.VMEM(fields.shape, f32),
            pltpu.VMEM(lines.shape, f32),
            pltpu.VMEM(mixing.shape, f32),
            pltpu.VMEM(bank.shape, f32),
            pltpu.VMEM((lay.total, channels), f32),
            pltpu.VMEM((rows, 2 * lay.count, 3 * pad), bf16),
            pltpu.VMEM((lay.total, channels), f32),
            pltpu.VMEM((rows, 3 * pad, channels), bf16),
            pltpu.VMEM((2, lay.tall, 3 * pad), bf16),
            pltpu.VMEM((4, rows, pad), f32),
            pltpu.VMEM((rows, 2 * pad), f32),
            pltpu.VMEM((rows, pad, 6 * lay.count), bf16),
            pltpu.SemaphoreType.DMA((3,)),
            pltpu.SemaphoreType.DMA((4,)),
            pltpu.SemaphoreType.DMA((rows // 2,)),
            pltpu.SemaphoreType.DMA((ring - 1, rows // 2)),
            pltpu.SemaphoreType.DMA((ring - 1, rows // 2)),
        ],
        compiler_params=pltpu.CompilerParams(collective_id=0, has_side_effects=True, vmem_limit_bytes=48 * 1024 * 1024),
        name="filter",
    )(*inputs)


def solution(mesh):
    return jax.shard_map(
        functools.partial(local, mesh.shape["lon"], mesh.shape["lat"]),
        mesh=mesh,
        in_specs=(P("lat", "lon", None), P("lat")),
        out_specs=P("lat", "lon", None),
        check_vma=False,
    )
```
